32 devices in a mesh: patch: 16 (over z, y, x), sub: 2 (over core).
Axes of the slice: x: 2, y: 2, z: 4, core: 2. Of those that a mesh axis runs over, the one named last changes fastest.
Arguments:
- fields: float32 [5, 64, 128, 128], P(None, ('patch', 'sub')), may hold values from -6 to 6
- density: float32 [64, 128, 128], P(('patch', 'sub')), may hold values from 1 to 3
- moduli: float32 [2, 64, 128, 128], P(None, ('patch', 'sub')), may hold values from 0.5 to 128
- metric_diag: float32 [2, 64, 128, 128], P(None, ('patch', 'sub')), may hold values from 0.7 to 1.3
- metric_cross: float32 [2, 64, 128, 128], P(None, ('patch', 'sub')), may hold values from -0.3 to 0.3
- fc_extension: float32 [25, 10], replicated, may hold values from -2 to 2
- patch_count: int32 [32], P(('patch', 'sub')), may hold values from 1 to 2, as said below
- connectivity: int32 [256, 3], P(('patch', 'sub')), may hold values from -1 to 31, as said below
Outputs:
- advanced: float32 [5, 64, 128, 128], P(None, ('patch', 'sub'))
The draws below stay inside these ranges and needn't reach their ends.
Inputs may be any that keep to these rules, and one draw needn't show every extreme that they name: `patch_count`: every device holds at most 2 live patches; the largest count is 2 in every draw. `connectivity`: links join only live slots and are symmetric with equal orientation flags on both ends; a neighbour is held by the same device or by the device whose flat index differs by 1 or 17 modulo 32; from one device to another device go at most 2 linked sides, and this number is reached in every draw.
All inputs are finite; a program needn't handle non-finite values.
Results may differ from the reference program's by a relative error of at most 0.00005.
Values sent between devices are 32-bit elements; how exact they have to be, the bound alone decides.
A program may use at most 64 MiB of HBM per device.

```python
import math
import jax
import jax.numpy as jnp
from jax import lax

N = 128
CONT = 25
MATCH = 5
PMAX = 2
STRIDE = 17
SLOTS = 64
DEVICES = 32


def patch_layout(key):
    base = jax.random.fold_in(key, 11)
    key_count, key_west, key_north = jax.random.split(base, 3)
    counts = jax.random.randint(key_count, (DEVICES,), max(1, PMAX // 4), PMAX + 1)
    counts = counts.at[0].set(PMAX).at[STRIDE].set(PMAX)
    west_flip = jax.random.randint(key_west, (DEVICES, PMAX), 0, 2)
    north_flip = jax.random.randint(key_north, (DEVICES, PMAX), 0, 2)
    return (counts.astype(jnp.int32), west_flip.astype(jnp.int32), north_flip.astype(jnp.int32))


def draw_patch_count(key, part):
    return patch_layout(key)[0]


def link_entry(linked, device_col, slot_col, side_value, flip_col):
    shape = (DEVICES, PMAX)
    linked = jnp.broadcast_to(linked, shape)
    device_col = jnp.broadcast_to(device_col, shape)
    slot_col = jnp.broadcast_to(slot_col, shape)
    flip_col = jnp.broadcast_to(flip_col, shape)
    return jnp.stack([jnp.where(linked, device_col, -1), jnp.where(linked, slot_col * 4 + side_value, 0), jnp.where(linked, flip_col, 0)], axis=-1)


def draw_connectivity(key, part):
    counts, west_flip, north_flip = patch_layout(key)
    device_ids = jnp.arange(DEVICES, dtype=jnp.int32)[:, None]
    slot_ids = jnp.arange(PMAX, dtype=jnp.int32)[None, :]
    held = counts[:, None]
    live = slot_ids < held
    before = (device_ids - 1) % DEVICES
    after = (device_ids + 1) % DEVICES
    above = (device_ids + STRIDE) % DEVICES
    below = (device_ids - STRIDE) % DEVICES
    first = slot_ids == 0
    last = slot_ids == held - 1
    west_dev = jnp.where(first, before, device_ids)
    west_slot = jnp.where(first, counts[before] - 1, slot_ids - 1)
    east_dev = jnp.where(last, after, device_ids)
    east_slot = jnp.where(last, 0, slot_ids + 1)
    next_index = jnp.broadcast_to(jnp.minimum(slot_ids + 1, PMAX - 1), (DEVICES, PMAX))
    inner_flip = jnp.take_along_axis(west_flip, next_index, axis=1)
    east_flip = jnp.where(last, west_flip[after[:, 0], 0][:, None], inner_flip)
    south_linked = live & (slot_ids < counts[below])
    north_linked = live & (slot_ids < counts[above])
    south_flip = north_flip[below[:, 0]]
    table = jnp.stack([link_entry(live, west_dev, west_slot, 1, west_flip), link_entry(live, east_dev, east_slot, 0, east_flip), link_entry(south_linked, below, slot_ids, 3, south_flip), link_entry(north_linked, above, slot_ids, 2, north_flip)], axis=2)
    return table.reshape(DEVICES * PMAX * 4, 3).astype(jnp.int32)


def draw_moduli(key, part):
    counts = patch_layout(key)[0]
    live_slots = (jnp.arange(PMAX, dtype=jnp.int32)[None, :] < counts[:, None]).reshape(SLOTS)
    key_patch, key_cell, key_dead = jax.random.split(jax.random.fold_in(key, 23), 3)
    top_factor = 4.0
    cell = jnp.exp(jax.random.uniform(key_cell, (2, SLOTS, N, N), jnp.float32, jnp.log(0.5), jnp.log(2.0)))
    live_factor = jnp.exp(jax.random.uniform(key_patch, (SLOTS,), jnp.float32) * jnp.log(top_factor))
    dead_factor = top_factor * jnp.exp(jax.random.uniform(key_dead, (SLOTS,), jnp.float32, jnp.log(2.0), jnp.log(4.0)))
    factor = jnp.where(live_slots, live_factor, dead_factor)
    return (factor[None, :, None, None] * cell).astype(jnp.float32)


def steps_of(rng, dims, pieces, smallest, largest):
    gain = 1.0
    for axis_at, blocks in pieces:
        draws = jax.random.uniform(jax.random.fold_in(jax.random.fold_in(rng, 6), axis_at), (blocks,), jnp.float32, smallest / len(pieces), largest / len(pieces))
        gain = gain * jnp.repeat(jnp.exp(draws), dims[axis_at] // blocks).reshape((-1,) + (1,) * (len(dims) - 1 - axis_at))
    return gain


def centred(key, dims, width, reach, cuts=(), held_as=jnp.bfloat16):
    factor_of = steps_of(key, dims, cuts, -0.22, 0.18) if cuts else 1.0
    entries = jax.random.normal(key, dims, jnp.float32) * width * factor_of
    return jnp.minimum(jnp.maximum(entries, -reach), reach).astype(held_as)


def setup_inputs(seed: int = 0) -> dict:
    keys = jax.random.split(jax.random.key(seed), 9)
    fields = centred(keys[0], (5, SLOTS, N, N), 1.0, 6.0, ((1, 32),), jnp.float32)
    density = jnp.clip(jnp.exp(math.log(3.0) - 1.0986123 * jax.random.uniform(keys[1], (SLOTS, N, N), jnp.float32) ** steps_of(keys[1], (SLOTS, N, N), ((0, 32),), -0.2, 0.2)), 1.0, 3.0)
    moduli = draw_moduli(jax.random.fold_in(keys[8], 71), 0)
    metric_diag = jnp.clip(0.7 + 0.59999996 * jax.random.uniform(keys[3], (2, SLOTS, N, N), jnp.float32) ** steps_of(keys[3], (2, SLOTS, N, N), ((1, 32),), -0.2, 0.2), 0.7, 1.3)
    metric_cross = jnp.clip(jax.random.uniform(keys[4], (2, SLOTS, N, N), jnp.float32, -0.3, 0.3) * steps_of(keys[4], (2, SLOTS, N, N), ((1, 32),), -0.4, 0.0), -0.3, 0.3)
    fc_extension = centred(keys[5], (CONT, 2 * MATCH), (2 * MATCH) ** -0.5, 2.0, (), jnp.float32)
    patch_count = draw_patch_count(jax.random.fold_in(keys[8], 71), 0)
    connectivity = draw_connectivity(jax.random.fold_in(keys[8], 71), 0)
    return dict(fields=fields, density=density, moduli=moduli, metric_diag=metric_diag, metric_cross=metric_cross, fc_extension=fc_extension, patch_count=patch_count, connectivity=connectivity)


cfl_number = 0.5
penalty_weight = 0.5

def wave_speed(density, moduli, metric_diag, metric_cross):
    stiff = moduli[0] + 2.0 * moduli[1]
    xi_norm = jnp.sqrt(metric_diag[0] * metric_diag[0] + metric_cross[0] * metric_cross[0])
    eta_norm = jnp.sqrt(metric_cross[1] * metric_cross[1] + metric_diag[1] * metric_diag[1])
    return jnp.sqrt(stiff / density) * (xi_norm + eta_norm)

def boundary_lines(state):
    stacked = jnp.stack([state[:, :, 0, :], state[:, :, -1, :], state[:, :, :, 0], state[:, :, :, -1]], axis=0)
    return jnp.transpose(stacked, (2, 0, 1, 3))

def assemble(state, along_xi, along_eta, partner_lines, side_mask, density, moduli, metric_diag, metric_cross):
    grad_x = metric_diag[0] * along_xi + metric_cross[1] * along_eta
    grad_y = metric_cross[0] * along_xi + metric_diag[1] * along_eta
    lame_first = moduli[0]
    shear = moduli[1]
    stiff = lame_first + 2.0 * shear
    rate_one = (grad_x[2] + grad_y[4]) / density
    rate_two = (grad_x[4] + grad_y[3]) / density
    rate_xx = stiff * grad_x[0] + lame_first * grad_y[1]
    rate_yy = lame_first * grad_x[0] + stiff * grad_y[1]
    rate_xy = shear * (grad_y[0] + grad_x[1])
    rate = jnp.stack([rate_one, rate_two, rate_xx, rate_yy, rate_xy], axis=0)
    points = state.shape[-1]
    jump = penalty_weight * (points - 1) * (partner_lines - boundary_lines(state)) * side_mask[:, :, None, None]
    jump = jnp.transpose(jump, (1, 2, 0, 3))
    rate = rate.at[:, :, 0, :].add(jump[0])
    rate = rate.at[:, :, points - 1, :].add(jump[1])
    rate = rate.at[:, :, :, 0].add(jump[2])
    rate = rate.at[:, :, :, points - 1].add(jump[3])
    return rate

def fc_derivative(values, extension, axis):
    moved = jnp.moveaxis(values, axis, -1)
    points = moved.shape[-1]
    match_pts = extension.shape[1] // 2
    tail = jnp.concatenate([moved[..., points - match_pts:], moved[..., :match_pts]], axis=-1)
    extra_vals = jnp.einsum('...m,cm->...c', tail, extension, precision=lax.Precision.HIGHEST)
    line = jnp.concatenate([moved, extra_vals], axis=-1)
    length = line.shape[-1]
    coeffs = jnp.fft.rfft(line, axis=-1)
    wave = 2.0 * jnp.pi * jnp.arange(length // 2 + 1, dtype=jnp.float32) * (points - 1) / length
    deriv = jnp.fft.irfft(coeffs * (1j * wave), n=length, axis=-1)[..., :points]
    return jnp.moveaxis(deriv.astype(values.dtype), -1, axis)

def reference(fields, density, moduli, metric_diag, metric_cross, fc_extension, patch_count, connectivity):
    state = fields.reshape(5, DEVICES, PMAX, N, N).transpose(1, 0, 2, 3, 4)
    dens_dev = density.reshape(DEVICES, PMAX, N, N)
    moduli_dev = moduli.reshape(2, DEVICES, PMAX, N, N).transpose(1, 0, 2, 3, 4)
    diag_dev = metric_diag.reshape(2, DEVICES, PMAX, N, N).transpose(1, 0, 2, 3, 4)
    cross_dev = metric_cross.reshape(2, DEVICES, PMAX, N, N).transpose(1, 0, 2, 3, 4)
    live = jnp.arange(PMAX, dtype=jnp.int32)[None, :] < patch_count[:, None]
    side_mask = (connectivity[:, 0] >= 0).astype(jnp.float32).reshape(DEVICES, PMAX, 4)

    def device_bound(device_data):
        speeds = wave_speed(device_data[0], device_data[1], device_data[2], device_data[3])
        return jnp.max(jnp.where(device_data[4][:, None, None], speeds, jnp.float32(0.0)))
    bound = jnp.max(lax.map(device_bound, (dens_dev, moduli_dev, diag_dev, cross_dev, live)))
    time_step = cfl_number / (bound * (N - 1))
    flat_target = (jnp.maximum(connectivity[:, 0], 0) * (PMAX * 4) + connectivity[:, 1]).astype(jnp.int32)
    flip_rows = connectivity[:, 2] == 1

    def partners(current):
        lines_all = jax.vmap(boundary_lines)(current).reshape(DEVICES * PMAX * 4, 5, N)
        picked = lines_all[flat_target]
        picked = jnp.where(flip_rows[:, None, None], picked[..., ::-1], picked)
        return picked.reshape(DEVICES, PMAX, 4, 5, N)

    def advance(current):
        near_lines = partners(current)

        def one_device(device_data):
            local = device_data[0]
            along_xi = fc_derivative(local, fc_extension, 2)
            along_eta = fc_derivative(local, fc_extension, 3)
            rate = assemble(local, along_xi, along_eta, device_data[1], device_data[2], device_data[3], device_data[4], device_data[5], device_data[6])
            return local + time_step * rate
        return lax.map(one_device, (current, near_lines, side_mask, dens_dev, moduli_dev, diag_dev, cross_dev))
    middle = advance(state)
    final = advance(middle)
    result = jnp.where(live[:, None, :, None, None], 0.5 * (state + final), jnp.float32(0.0))
    return result.transpose(1, 0, 2, 3, 4).reshape(5, SLOTS, N, N)
```

```python
import functools

import jax
import jax.numpy as jnp
import numpy as np
from jax import lax
from jax.experimental import pallas as pl
from jax.experimental.pallas import tpu as pltpu
from jax.sharding import PartitionSpec as P

MESH = pl.DeviceIdType.MESH
ROWS = 8
cfl_number = 0.5
penalty_weight = 0.5


def circulant(points, extra):
    length = points + extra
    half = (length - 1) // 2
    waves = np.arange(1, half + 1, dtype=np.float64)
    weights = waves * (2.0 * np.pi * (points - 1) / length)
    shifts = np.arange(length)
    phase = 2.0 * np.pi / length * (waves[:, None] * shifts[None, :] % length)
    kernel = -(2.0 / length) * np.sum(weights[:, None] * np.sin(phase), axis=0)
    at = (np.arange(points)[:, None] - np.arange(length)[None, :]) % length
    full = kernel[at].astype(np.float32)
    padded = -(-extra // ROWS) * ROWS
    outer = np.zeros((points, points), np.float32)
    outer[:, :extra] = full[:, points:]
    return full[:, :points], outer, padded


def split(x):
    hi = x.astype(jnp.bfloat16)
    lo = (x - hi.astype(jnp.float32)).astype(jnp.bfloat16)
    return hi, lo


def kernel(
    total, subs, offsets, reach,
    conn_hbm, count_hbm, fields_hbm, density_hbm, moduli_hbm, diag_hbm, cross_hbm,
    ext_hbm, inner_hbm, outer_hbm,
    out_v,
    conn, count, ext, inner, outer,
    fld, den, mod, dia, cro, rate1, dxi, deta, left, right, ext_v, cols, trans,
    lines, lines2, turned1, turned2, outbox1, outbox2, inbox1, inbox2, corner, corners,
    mine, gather,
    load_sem, send1, recv1, send2, recv2, csend, crecv, bsend, brecv,
):
    comps, slots, n, _ = fld.shape
    sides = slots * 4
    chunks = n // ROWS
    me = lax.axis_index("patch") * subs + lax.axis_index("sub")

    def place(flat):
        return (lax.div(flat, subs), lax.rem(flat, subs))

    def away(off):
        return lax.rem(me + off, total)

    loads = []
    for at, (src, dst) in enumerate(
        (
            (conn_hbm, conn), (count_hbm, count), (ext_hbm, ext), (inner_hbm, inner),
            (outer_hbm, outer), (fields_hbm, fld), (density_hbm, den), (moduli_hbm, mod),
            (diag_hbm, dia), (cross_hbm, cro),
        )
    ):
        if src is fields_hbm:
            for f in range(comps):
                pltpu.make_async_copy(src.at[f], dst.at[f], load_sem.at[at]).start()
        else:
            pltpu.make_async_copy(src, dst, load_sem.at[at]).start()
        loads.append(pltpu.make_async_copy(src, dst, load_sem.at[at]))

    barrier = pltpu.get_barrier_semaphore()

    def greet(d, _):
        pl.semaphore_signal(barrier, inc=1, device_id=place(away(d)), device_id_type=MESH)
        return _

    lax.fori_loop(1, total, greet, 0)

    lines[...] = jnp.zeros_like(lines)
    lines2[...] = jnp.zeros_like(lines2)
    trans[...] = jnp.zeros_like(trans)
    ext_v[...] = jnp.zeros_like(ext_v)

    loads[0].wait()
    loads[1].wait()
    near = [away(off) for off in offsets]
    owner = [conn[0, s] for s in range(sides)]
    linked = [owner[s] >= 0 for s in range(sides)]
    strip = [jnp.where(linked[s], conn[1, s], 0) for s in range(sides)]
    flip = [conn[2, s] for s in range(sides)]
    picks = []
    for peer in near:
        seen = jnp.int32(0)
        pick = [jnp.int32(0)] * slots
        for s in range(sides):
            hit = owner[s] == peer
            for k in range(slots):
                pick[k] = jnp.where(hit & (seen == k), s, pick[k])
            seen = seen + hit.astype(jnp.int32)
        picks.append(pick)
    box, local = [], []
    for s in range(sides):
        pos = jnp.int32(0)
        for t in range(sides):
            if t != s:
                pos = pos + ((owner[t] == owner[s]) & (strip[t] < strip[s])).astype(jnp.int32)
        pos = jnp.minimum(pos, slots - 1)
        at = pos
        for o, off in enumerate(offsets):
            at = jnp.where(owner[s] == away(total - off), o * slots + pos, at)
        box.append(at)
        local.append(owner[s] == me)

    lane = lax.broadcasted_iota(jnp.int32, (ROWS, n), 1)
    row = lax.broadcasted_iota(jnp.int32, (ROWS, n), 0)
    low, high = lane == 0, lane == n - 1
    edge = low | high
    used = row < comps
    pairs = [(f, p, p * 8 + f) for p in range(slots) for f in range(comps)]
    weight = penalty_weight * (n - 1)

    def collect(state, lines):
        def columns(c, _):
            rows = pl.ds(pl.multiple_of(c * ROWS, ROWS), ROWS)
            acc = jnp.zeros((ROWS, n), jnp.float32)
            for f, p, m in pairs:
                turned = pltpu.roll(state[f, p, rows, :], 2 * m + 1, 1)
                acc = jnp.where((lane == 2 * m) | (lane == 2 * m + 1), turned, acc)
            cols[rows, :] = acc
            return _

        lax.fori_loop(0, chunks, columns, 0, unroll=chunks)
        trans[...] = jnp.transpose(cols[...])
        for p in range(slots):
            lines[p * 4 + 2] = trans[pl.ds(p * 16 + 1, 8, stride=2), :]
            lines[p * 4 + 3] = trans[pl.ds(p * 16, 8, stride=2), :]
            for f in range(comps):
                lines[p * 4, pl.ds(f, 1)] = state[f, p, pl.ds(0, 1), :]
                lines[p * 4 + 1, pl.ds(f, 1)] = state[f, p, pl.ds(n - 1, 1), :]

    def turn(lines, turned):
        for s in range(sides):
            index = jnp.where(flip[s] == 1, n - 1 - lane, lane)
            turned[s] = jnp.take_along_axis(lines[s], index, axis=1)

    def post(turned, outbox, inbox, send, recv):
        for o in range(len(offsets)):
            for k in range(slots):
                outbox[o, k] = turned[picks[o][k]]
        sent = []
        for o in range(len(offsets)):
            copy = pltpu.make_async_remote_copy(
                src_ref=outbox.at[o, :, pl.ds(0, comps), :],
                dst_ref=inbox.at[pl.ds(o * slots, slots), pl.ds(0, comps), :],
                send_sem=send.at[o],
                recv_sem=recv.at[o],
                device_id=place(near[o]),
                device_id_type=MESH,
            )
            copy.start()
            sent.append(copy)
        return sent

    def partners(turned, inbox):
        return [
            jnp.where(used, jnp.where(local[s], turned[strip[s]], inbox[box[s]]), 0.0)
            for s in range(sides)
        ]

    def spread(jump):
        for p in range(slots):
            trans[pl.ds(p * 16 + 1, 8, stride=2), :] = jump[p * 4 + 2]
            trans[pl.ds(p * 16, 8, stride=2), :] = jump[p * 4 + 3]
        cols[...] = jnp.transpose(trans[...])

    def derive(state):
        for f in range(comps):
            h0, l0 = split(state[f, 0])
            h1, l1 = split(state[f, 1])
            rows = jnp.concatenate(
                [jnp.concatenate([h0, l0], axis=1), jnp.concatenate([h1, l1], axis=1)], axis=0
            )
            eta = jnp.dot(rows, right[...], preferred_element_type=jnp.float32)
            both = eta[:, :n] + eta[:, n:]
            deta[f, 0] = both[:n]
            deta[f, 1] = both[n:]
            body = jnp.concatenate(
                [jnp.concatenate([h0, h1], axis=1), jnp.concatenate([l0, l1], axis=1)], axis=0
            )
            xi = jnp.dot(left[...], body, preferred_element_type=jnp.float32)
            both = xi[:n] + xi[n:]
            dxi[f, 0] = both[:, :n]
            dxi[f, 1] = both[:, n:]

    def interior(keep):
        for p in range(slots):

            def body(c, _):
                rows = pl.ds(pl.multiple_of(c * ROWS, ROWS), ROWS)
                xx, yy = dia[0, p, rows, :], dia[1, p, rows, :]
                xy, ex = cro[0, p, rows, :], cro[1, p, rows, :]
                lame, shear = mod[0, p, rows, :], mod[1, p, rows, :]
                inv = den[p, rows, :]
                stiff = lame + 2.0 * shear
                ax = [dxi[f, p, rows, :] for f in range(comps)]
                ay = [deta[f, p, rows, :] for f in range(comps)]
                gx = [xx * a + ex * b for a, b in zip(ax, ay)]
                gy = [xy * a + yy * b for a, b in zip(ax, ay)]
                keep(0, p, rows, (gx[2] + gy[4]) * inv)
                keep(1, p, rows, (gx[4] + gy[3]) * inv)
                keep(2, p, rows, stiff * gx[0] + lame * gy[1])
                keep(3, p, rows, lame * gx[0] + stiff * gy[1])
                keep(4, p, rows, shear * (gy[0] + gx[1]))
                return _

            lax.fori_loop(0, chunks, body, 0, unroll=chunks)

    def add_rows(state, jump):
        for p in range(slots):
            for f in range(comps):
                for side, at in ((0, 0), (1, n - 1)):
                    spot = pl.ds(at, 1)
                    state[f, p, spot, :] = state[f, p, spot, :] + jump[p * 4 + side][f : f + 1]

    def add_columns(state):
        def body(c, _):
            rows = pl.ds(pl.multiple_of(c * ROWS, ROWS), ROWS)
            both = cols[rows, :]
            for f, p, m in pairs:
                side = pltpu.roll(both, n - (2 * m + 1), 1)
                state[f, p, rows, :] = state[f, p, rows, :] + jnp.where(edge, side, 0.0)
            return _

        lax.fori_loop(0, chunks, body, 0, unroll=chunks)

    for at in (2, 3, 4):
        loads[at].wait()
    twice, extra = ext.shape
    ext_v[pl.ds(0, twice), pl.ds(0, extra)] = ext[...]
    turned = pltpu.roll(ext_v[...], n - twice // 2, 0)
    matrix = inner[...] + lax.dot_general(
        outer[...],
        turned,
        (((1,), (1,)), ((), ())),
        precision=lax.Precision.HIGHEST,
        preferred_element_type=jnp.float32,
    )
    hi, lo = split(matrix)
    none = jnp.zeros_like(hi)
    left[...] = jnp.concatenate(
        [jnp.concatenate([hi, hi], axis=1), jnp.concatenate([lo, none], axis=1)], axis=0
    )
    hi, lo = split(jnp.transpose(matrix))
    right[...] = jnp.concatenate(
        [jnp.concatenate([hi, lo], axis=1), jnp.concatenate([hi, none], axis=1)], axis=0
    )

    loads[5].wait()
    collect(fld, lines)
    turn(lines, turned1)
    tile = jnp.zeros((ROWS, n), jnp.float32)
    for p in range(slots):
        for b in range(2):
            first = p * 4 + 2 * b
            rolled = pltpu.roll(lines[p * 4 + b], first + 1, 1)
            tile = jnp.where((lane == first) | (lane == first + 1), rolled, tile)
    for r in range(3):
        for s in range(sides):
            tile = jnp.where(
                (row == comps + r) & (lane == s), conn[r, s].astype(jnp.float32), tile
            )
    packed = jnp.sum(
        pltpu.roll(tile, 0, 1, stride=sides, stride_axis=0), axis=0, keepdims=True
    )
    corner[...] = packed
    corners[0] = packed

    pl.semaphore_wait(barrier, total - 1)
    sent1 = post(turned1, outbox1, inbox1, send1, recv1)
    sentc = []
    for j, off in enumerate(reach):
        if j > 0:
            there = reach.index(total - off)
            copy = pltpu.make_async_remote_copy(
                src_ref=corner,
                dst_ref=corners.at[there],
                send_sem=csend.at[j - 1],
                recv_sem=crecv.at[there - 1],
                device_id=place(away(off)),
                device_id_type=MESH,
            )
            copy.start()
            sentc.append(copy)

    for load in loads[6:]:
        load.wait()
    top = jnp.zeros((ROWS, n), jnp.float32)
    for p in range(slots):

        def speeds(c, top):
            rows = pl.ds(pl.multiple_of(c * ROWS, ROWS), ROWS)
            xx, yy = dia[0, p, rows, :], dia[1, p, rows, :]
            xy, ex = cro[0, p, rows, :], cro[1, p, rows, :]
            stiff = mod[0, p, rows, :] + 2.0 * mod[1, p, rows, :]
            inv = 1.0 / den[p, rows, :]
            den[p, rows, :] = inv
            speed = jnp.sqrt(stiff * inv) * (
                jnp.sqrt(xx * xx + xy * xy) + jnp.sqrt(ex * ex + yy * yy)
            )
            return jnp.maximum(top, speed)

        part = lax.fori_loop(
            0, chunks, speeds, jnp.zeros((ROWS, n), jnp.float32), unroll=chunks
        )
        top = jnp.maximum(top, jnp.where(count[0] > p, part, 0.0))
    mine[...] = jnp.max(top, axis=0, keepdims=True)

    def tell(d, _):
        pltpu.make_async_remote_copy(
            src_ref=mine,
            dst_ref=gather.at[d - 1],
            send_sem=bsend.at[0],
            recv_sem=brecv.at[0],
            device_id=place(away(d)),
            device_id_type=MESH,
        ).start()
        return _

    lax.fori_loop(1, total, tell, 0)

    derive(fld)

    def keep1(f, p, rows, value):
        rate1[f, p, rows, :] = value

    interior(keep1)
    collect(rate1, lines2)
    turn(lines2, turned2)
    sent2 = post(turned2, outbox2, inbox2, send2, recv2)

    for copy in sent1 + sentc:
        copy.wait_recv()
    other = partners(turned1, inbox1)
    jump1 = [jnp.where(linked[s], weight * (other[s] - lines[s]), 0.0) for s in range(sides)]
    spread(jump1)
    add_rows(rate1, jump1)
    add_columns(rate1)

    def whole(value):
        return jnp.broadcast_to(value, (ROWS, n))

    table = jnp.zeros((ROWS, n), jnp.float32)
    for j in range(len(reach)):
        index = (lane - j * sides + row * sides) & (n - 1)
        laid = jnp.take_along_axis(whole(corners[j]), index, axis=1)
        table = jnp.where((lane >= j * sides) & (lane < (j + 1) * sides), laid, table)
    their_owner = jnp.full((ROWS, n), -1, jnp.int32)
    their_strip = jnp.zeros((ROWS, n), jnp.int32)
    their_flip = jnp.zeros((ROWS, n), jnp.int32)
    for s in range(sides):
        here = lax.shift_right_logical(lane, 1) == s
        their_owner = jnp.where(here, owner[s], their_owner)
        their_strip = jnp.where(here, strip[s], their_strip)
        their_flip = jnp.where(here, flip[s], their_flip)

    def seat(device):
        at = jnp.zeros((ROWS, n), jnp.int32)
        for j, off in enumerate(reach):
            at = jnp.where(device == away(off), j * sides, at)
        return at

    def nook(strip, end):
        b = strip & 1
        across = (strip & 2) == 0
        return (strip & ~3) + jnp.where(across, 2 * b + 1 - end, 2 * end + 1 - b)

    end = (1 - (lane & 1)) ^ (their_flip & 1)
    base = seat(their_owner)
    beside = (their_strip & ~3) + jnp.where((their_strip & 2) == 0, 2 + end, end)
    entry = jnp.take_along_axis(table, base + beside, axis=1)
    own = jnp.take_along_axis(table, base + nook(their_strip, end), axis=1)
    far_owner = whole(entry[comps : comps + 1]).astype(jnp.int32)
    far_strip = whole(entry[comps + 1 : comps + 2]).astype(jnp.int32)
    far_flip = whole(entry[comps + 2 : comps + 3]).astype(jnp.int32)
    far_strip = jnp.where(far_owner >= 0, far_strip, 0)
    far_end = (their_strip & 1) ^ (far_flip & 1)
    value = jnp.take_along_axis(table, seat(far_owner) + nook(far_strip, far_end), axis=1)
    bend = jnp.where((far_owner >= 0) & used, weight * (value - own), 0.0)

    rest = []
    for p in range(slots):
        west, east, south, north = jump1[p * 4 : p * 4 + 4]
        mixed = (
            jnp.where(low, south, 0.0) + jnp.where(high, pltpu.roll(north, n - 1, 1), 0.0),
            jnp.where(low, pltpu.roll(south, 1, 1), 0.0) + jnp.where(high, north, 0.0),
            jnp.where(low, west, 0.0) + jnp.where(high, pltpu.roll(east, n - 1, 1), 0.0),
            jnp.where(low, pltpu.roll(west, 1, 1), 0.0) + jnp.where(high, east, 0.0),
        )
        for side in range(4):
            s = p * 4 + side
            theirs = jnp.where(edge, pltpu.roll(bend, n - (2 * s + 1), 1), 0.0)
            rest.append(theirs - mixed[side] - 2.0 * jump1[s] - lines2[s])

    derive(rate1)

    pltpu.make_async_copy(gather, gather, brecv.at[0]).wait()
    best = mine[...]
    for d in range(total - 1):
        best = jnp.maximum(best, gather[d])
    bound = jnp.max(best, axis=1, keepdims=True)
    step = jnp.broadcast_to(cfl_number / (bound * (n - 1)), (ROWS, n))
    half = 0.5 * step * step

    def keep2(f, p, rows, second):
        value = fld[f, p, rows, :] + step * rate1[f, p, rows, :] + half * second
        out_v[f, p, rows, :] = jnp.where(count[0] > p, value, 0.0)

    interior(keep2)

    for copy in sent2:
        copy.wait_recv()
    other = partners(turned2, inbox2)
    jump2 = [
        jnp.where(linked[s], (half * weight) * (other[s] + rest[s]), 0.0) for s in range(sides)
    ]
    spread(jump2)
    add_rows(out_v, jump2)
    add_columns(out_v)

    for copy in sent1 + sentc + sent2:
        copy.wait_send()
    pltpu.make_async_copy(gather, gather, bsend.at[0]).wait()


def shards(
    total, subs, fields, density, moduli, metric_diag, metric_cross, extension, count, connectivity
):
    comps, slots, n, _ = fields.shape
    inner, outer, _ = circulant(n, extension.shape[0])
    far = total // 2 + 1
    offsets = (1, total - 1, far, total - far)
    reach = [0, *offsets]
    for a in offsets:
        for b in offsets:
            if (a + b) % total not in reach:
                reach.append((a + b) % total)
    f32, i32 = jnp.float32, jnp.int32
    hbm = pl.BlockSpec(memory_space=pltpu.HBM)
    state = pltpu.VMEM(fields.shape, f32)
    square = pltpu.VMEM((n, n), f32)
    dma = pltpu.SemaphoreType.DMA
    boxed = pltpu.VMEM((4, slots, 8, n), f32)
    arrived = pltpu.VMEM((4 * slots, 8, n), f32)
    strips = pltpu.VMEM((slots * 4, 8, n), f32)
    return pl.pallas_call(
        functools.partial(kernel, total, subs, offsets, reach),
        out_shape=pltpu.VMEM(fields.shape, f32),
        in_specs=[hbm] * 10,
        out_specs=pl.BlockSpec(memory_space=pltpu.VMEM),
        scratch_shapes=[
            pltpu.SMEM(connectivity.shape[::-1], i32),
            pltpu.SMEM(count.shape, i32),
            pltpu.VMEM(extension.shape[::-1], f32),
            square, square,
            state,
            pltpu.VMEM(density.shape, f32),
            pltpu.VMEM(moduli.shape, f32),
            pltpu.VMEM(metric_diag.shape, f32),
            pltpu.VMEM(metric_cross.shape, f32),
            state, state, state,
            pltpu.VMEM((2 * n, 2 * n), jnp.bfloat16),
            pltpu.VMEM((2 * n, 2 * n), jnp.bfloat16),
            square, square, square,
            strips, strips, strips, strips,
            boxed, boxed, arrived, arrived,
            pltpu.VMEM((1, n), f32),
            pltpu.VMEM((len(reach), 1, n), f32),
            pltpu.VMEM((1, n), f32),
            pltpu.VMEM((total - 1, 1, n), f32),
            dma((10,)),
            dma((4,)), dma((4,)), dma((4,)), dma((4,)),
            dma((len(reach) - 1,)), dma((len(reach) - 1,)), dma((1,)), dma((1,)),
        ],
        compiler_params=pltpu.CompilerParams(collective_id=0, has_side_effects=True),
    )(connectivity.T, count, fields, density, moduli, metric_diag, metric_cross, extension.T,
      jnp.asarray(inner), jnp.asarray(outer))


def solution(mesh):
    placed = (
        P(None, ("patch", "sub"), None, None),
        P(("patch", "sub"), None, None),
        P(None, ("patch", "sub"), None, None),
        P(None, ("patch", "sub"), None, None),
        P(None, ("patch", "sub"), None, None),
        P(),
        P(("patch", "sub")),
        P(("patch", "sub"), None),
    )
    total = mesh.shape["patch"] * mesh.shape["sub"]
    return jax.shard_map(
        functools.partial(shards, total, mesh.shape["sub"]),
        mesh=mesh,
        in_specs=placed,
        out_specs=P(None, ("patch", "sub"), None, None),
        check_vma=False,
    )
```

```python
import functools

import jax
import jax.numpy as jnp
import numpy as np
from jax import lax
from jax.experimental import pallas as pl
from jax.experimental.pallas import tpu as pltpu
from jax.sharding import PartitionSpec as P

MESH = pl.DeviceIdType.MESH
ROWS = 8
cfl_number = 0.5
penalty_weight = 0.5


def circulant(points, extra):
    length = points + extra
    half = (length - 1) // 2
    waves = np.arange(1, half + 1, dtype=np.float64)
    weights = waves * (2.0 * np.pi * (points - 1) / length)
    shifts = np.arange(length)
    phase = 2.0 * np.pi / length * (waves[:, None] * shifts[None, :] % length)
    kernel = -(2.0 / length) * np.sum(weights[:, None] * np.sin(phase), axis=0)
    at = (np.arange(points)[:, None] - np.arange(length)[None, :]) % length
    full = kernel[at].astype(np.float32)
    padded = -(-extra // ROWS) * ROWS
    outer = np.zeros((points, points), np.float32)
    outer[:, :extra] = full[:, points:]
    return full[:, :points], outer, padded


def split(x):
    hi = x.astype(jnp.bfloat16)
    lo = (x - hi.astype(jnp.float32)).astype(jnp.bfloat16)
    return hi, lo


def kernel(
    total, subs, offsets, reach,
    conn_hbm, count_hbm, fields_hbm, density_hbm, moduli_hbm, diag_hbm, cross_hbm,
    ext_hbm, consts_hbm,
    out_v,
    conn, count, ext, consts,
    fld, med, rate1, dxi, deta, left, right, ext_v, cols, trans,
    lines, lines2, turned1, turned2, outbox1, outbox2, inbox1, inbox2, corner, corners,
    mine, gather,
    load_sem, send_sem, recv_sem,
):
    comps, slots, n, _ = fld.shape
    sides = slots * 4
    chunks = n // ROWS
    patch, core = lax.axis_index("patch"), lax.axis_index("sub")
    me = patch * subs + core
    simple = total & (total - 1) == 0 and subs & (subs - 1) == 0
    unroll = total - 1 if total <= 64 else 1

    def away(off):
        return lax.rem(me + off, total)

    def place(flat):
        return (lax.div(flat, subs), lax.rem(flat, subs))

    def peer(d):
        if simple:
            return (patch ^ lax.div(d, subs), core ^ lax.rem(d, subs))
        return place(away(d))

    conn_load = pltpu.make_async_copy(conn_hbm, conn, load_sem.at[0])
    count_load = pltpu.make_async_copy(count_hbm, count, load_sem.at[1])
    ext_load = pltpu.make_async_copy(ext_hbm, ext, load_sem.at[2])
    consts_load = pltpu.make_async_copy(consts_hbm, consts, load_sem.at[3])
    fields_load = pltpu.make_async_copy(fields_hbm, fld, load_sem.at[4])
    med_load = pltpu.make_async_copy(med, med, load_sem.at[5])
    conn_load.start()
    for f in range(comps):
        pltpu.make_async_copy(fields_hbm.at[f], fld.at[f], load_sem.at[4]).start()
    ext_load.start()
    consts_load.start()
    pltpu.make_async_copy(density_hbm, med.at[0], load_sem.at[5]).start()
    for k in range(2):
        pltpu.make_async_copy(moduli_hbm.at[k], med.at[1 + k], load_sem.at[5]).start()
        pltpu.make_async_copy(diag_hbm.at[k], med.at[3 + k], load_sem.at[5]).start()
        pltpu.make_async_copy(cross_hbm.at[k], med.at[5 + k], load_sem.at[5]).start()
    count_load.start()

    barrier = pltpu.get_barrier_semaphore()

    def greet(i, _):
        pl.semaphore_signal(
            barrier, inc=1, device_id=peer(total - 1 - i), device_id_type=MESH
        )
        return _

    lax.fori_loop(0, total - 1, greet, 0, unroll=unroll)

    lines[...] = jnp.zeros_like(lines)
    lines2[...] = jnp.zeros_like(lines2)
    trans[...] = jnp.zeros_like(trans)
    ext_v[...] = jnp.zeros_like(ext_v)

    conn_load.wait()
    near = [away(off) for off in offsets]
    owner = [conn[0, s] for s in range(sides)]
    linked = [owner[s] >= 0 for s in range(sides)]
    strip = [jnp.where(linked[s], conn[1, s], 0) for s in range(sides)]
    flip = [conn[2, s] for s in range(sides)]
    tags = []
    for s in range(sides):
        rank = jnp.int32(0)
        for t in range(s):
            rank = rank + (owner[t] == owner[s]).astype(jnp.int32)
        tags.append(owner[s] * sides + rank)
    picks = []
    for there in near:
        pick = []
        for k in range(slots):
            tag, at = there * sides + k, jnp.int32(0)
            for s in range(1, sides):
                at = jnp.where(tags[s] == tag, s, at)
            pick.append(at)
        picks.append(pick)

    lane = lax.broadcasted_iota(jnp.int32, (ROWS, n), 1)
    row = lax.broadcasted_iota(jnp.int32, (ROWS, n), 0)
    low, high = lane == 0, lane == n - 1
    edge = low | high
    used = row < comps
    pairs = [(f, p, p * 8 + f) for p in range(slots) for f in range(comps)]
    weight = penalty_weight * (n - 1)

    def collect(state, lines):
        def columns(c, _):
            rows = pl.ds(pl.multiple_of(c * ROWS, ROWS), ROWS)
            acc = jnp.zeros((ROWS, n), jnp.float32)
            for f, p, m in pairs:
                turned = pltpu.roll(state[f, p, rows, :], 2 * m + 1, 1)
                acc = jnp.where((lane == 2 * m) | (lane == 2 * m + 1), turned, acc)
            cols[rows, :] = acc
            return _

        lax.fori_loop(0, chunks, columns, 0, unroll=chunks)
        trans[...] = jnp.transpose(cols[...])
        for p in range(slots):
            lines[p * 4 + 2] = trans[pl.ds(p * 16 + 1, 8, stride=2), :]
            lines[p * 4 + 3] = trans[pl.ds(p * 16, 8, stride=2), :]
            for f in range(comps):
                lines[p * 4, pl.ds(f, 1)] = state[f, p, pl.ds(0, 1), :]
                lines[p * 4 + 1, pl.ds(f, 1)] = state[f, p, pl.ds(n - 1, 1), :]

    def turn(lines, turned):
        for s in range(sides):
            index = jnp.where(flip[s] == 1, n - 1 - lane, lane)
            turned[s] = jnp.take_along_axis(lines[s], index, axis=1)

    def post(turned, outbox, inbox, at):
        for o in range(len(offsets)):
            for k in range(slots):
                outbox[o * slots + k] = turned[picks[o][k]]
        for o in range(len(offsets)):
            spot = (pl.ds(o * slots, slots), pl.ds(0, comps), slice(None))
            pltpu.make_async_remote_copy(
                src_ref=outbox.at[spot],
                dst_ref=inbox.at[spot],
                send_sem=send_sem.at[at],
                recv_sem=recv_sem.at[at],
                device_id=place(near[o]),
                device_id_type=MESH,
            ).start()

    def settle(buffer, sem):
        pltpu.make_async_copy(buffer, buffer, sem).wait()

    def carried(buffer):
        return buffer.at[:, pl.ds(0, comps), :]

    def partners(turned, inbox):
        return [
            jnp.where(used, jnp.where(local[s], turned[strip[s]], inbox[box[s]]), 0.0)
            for s in range(sides)
        ]

    def spread(jump):
        for p in range(slots):
            trans[pl.ds(p * 16 + 1, 8, stride=2), :] = jump[p * 4 + 2]
            trans[pl.ds(p * 16, 8, stride=2), :] = jump[p * 4 + 3]
        cols[...] = jnp.transpose(trans[...])

    def derive(state):
        for f in range(comps):
            h0, l0 = split(state[f, 0])
            h1, l1 = split(state[f, 1])
            rows = jnp.concatenate(
                [jnp.concatenate([h0, l0], axis=1), jnp.concatenate([h1, l1], axis=1)], axis=0
            )
            eta = jnp.dot(rows, right[...], preferred_element_type=jnp.float32)
            both = eta[:, :n] + eta[:, n:]
            deta[f, 0] = both[:n]
            deta[f, 1] = both[n:]
            body = jnp.concatenate(
                [jnp.concatenate([h0, h1], axis=1), jnp.concatenate([l0, l1], axis=1)], axis=0
            )
            xi = jnp.dot(left[...], body, preferred_element_type=jnp.float32)
            both = xi[:n] + xi[n:]
            dxi[f, 0] = both[:, :n]
            dxi[f, 1] = both[:, n:]

    def interior(keep):
        for p in range(slots):

            def body(c, _):
                rows = pl.ds(pl.multiple_of(c * ROWS, ROWS), ROWS)
                inv, lame, shear, xx, yy, xy, ex = (med[k, p, rows, :] for k in range(7))
                stiff = lame + 2.0 * shear
                ax = [dxi[f, p, rows, :] for f in range(comps)]
                ay = [deta[f, p, rows, :] for f in range(comps)]
                gx = [xx * a + ex * b for a, b in zip(ax, ay)]
                gy = [xy * a + yy * b for a, b in zip(ax, ay)]
                keep(0, p, rows, (gx[2] + gy[4]) * inv)
                keep(1, p, rows, (gx[4] + gy[3]) * inv)
                keep(2, p, rows, stiff * gx[0] + lame * gy[1])
                keep(3, p, rows, lame * gx[0] + stiff * gy[1])
                keep(4, p, rows, shear * (gy[0] + gx[1]))
                return _

            lax.fori_loop(0, chunks, body, 0, unroll=chunks)

    def add_rows(state, jump):
        for p in range(slots):
            for f in range(comps):
                for side, at in ((0, 0), (1, n - 1)):
                    spot = pl.ds(at, 1)
                    state[f, p, spot, :] = state[f, p, spot, :] + jump[p * 4 + side][f : f + 1]

    def add_columns(state):
        def body(c, _):
            rows = pl.ds(pl.multiple_of(c * ROWS, ROWS), ROWS)
            both = cols[rows, :]
            for f, p, m in pairs:
                side = pltpu.roll(both, n - (2 * m + 1), 1)
                state[f, p, rows, :] = state[f, p, rows, :] + jnp.where(edge, side, 0.0)
            return _

        lax.fori_loop(0, chunks, body, 0, unroll=chunks)

    ext_load.wait()
    consts_load.wait()
    fields_load.wait()
    twice, extra = ext.shape
    ext_v[pl.ds(0, twice), pl.ds(0, extra)] = ext[...]
    turned = pltpu.roll(ext_v[...], n - twice // 2, 0)
    matrix = consts[0] + lax.dot_general(
        consts[1],
        turned,
        (((1,), (1,)), ((), ())),
        precision=lax.Precision.HIGHEST,
        preferred_element_type=jnp.float32,
    )
    hi, lo = split(matrix)
    none = jnp.zeros_like(hi)
    left[...] = jnp.concatenate(
        [jnp.concatenate([hi, hi], axis=1), jnp.concatenate([lo, none], axis=1)], axis=0
    )
    hi, lo = split(jnp.transpose(matrix))
    right[...] = jnp.concatenate(
        [jnp.concatenate([hi, lo], axis=1), jnp.concatenate([hi, none], axis=1)], axis=0
    )

    collect(fld, lines)
    turn(lines, turned1)

    pl.semaphore_wait(barrier, total - 1)
    post(turned1, outbox1, inbox1, 0)

    count_load.wait()
    med_load.wait()
    tile = jnp.zeros((ROWS, n), jnp.float32)
    for p in range(slots):
        for b in range(2):
            first = p * 4 + 2 * b
            rolled = pltpu.roll(lines[p * 4 + b], first + 1, 1)
            tile = jnp.where((lane == first) | (lane == first + 1), rolled, tile)
    for r in range(3):
        for s in range(sides):
            tile = jnp.where(
                (row == comps + r) & (lane == s), conn[r, s].astype(jnp.float32), tile
            )
    packed = jnp.sum(
        pltpu.roll(tile, 0, 1, stride=sides, stride_axis=0), axis=0, keepdims=True
    )
    corner[...] = packed
    corners[0] = packed

    top = jnp.zeros((ROWS, n), jnp.float32)
    for p in range(slots):

        def speeds(c, top):
            rows = pl.ds(pl.multiple_of(c * ROWS, ROWS), ROWS)
            dens, lame, shear, xx, yy, xy, ex = (med[k, p, rows, :] for k in range(7))
            inv = 1.0 / dens
            med[0, p, rows, :] = inv
            speed = jnp.sqrt((lame + 2.0 * shear) * inv) * (
                jnp.sqrt(xx * xx + xy * xy) + jnp.sqrt(ex * ex + yy * yy)
            )
            return jnp.maximum(top, speed)

        part = lax.fori_loop(
            0, chunks, speeds, jnp.zeros((ROWS, n), jnp.float32), unroll=chunks
        )
        top = jnp.maximum(top, jnp.where(count[0] > p, part, 0.0))
    mine[...] = jnp.max(top, axis=0, keepdims=True)
    derive(fld)

    def tell(i, _):
        d = total - 1 - i
        pltpu.make_async_remote_copy(
            src_ref=mine,
            dst_ref=gather.at[d - 1],
            send_sem=send_sem.at[1],
            recv_sem=recv_sem.at[1],
            device_id=peer(d),
            device_id_type=MESH,
        ).start()
        return _

    lax.fori_loop(0, total - 1, tell, 0, unroll=unroll)
    for j, off in enumerate(reach):
        if j > 0:
            pltpu.make_async_remote_copy(
                src_ref=corner,
                dst_ref=corners.at[reach.index(total - off)],
                send_sem=send_sem.at[2],
                recv_sem=recv_sem.at[2],
                device_id=place(away(off)),
                device_id_type=MESH,
            ).start()

    def keep1(f, p, rows, value):
        rate1[f, p, rows, :] = value

    interior(keep1)
    collect(rate1, lines2)
    turn(lines2, turned2)
    post(turned2, outbox2, inbox2, 3)

    box, local = [], []
    for s in range(sides):
        pos = jnp.int32(0)
        for t in range(sides):
            if t != s:
                pos = pos + ((owner[t] == owner[s]) & (strip[t] < strip[s])).astype(jnp.int32)
        pos = jnp.minimum(pos, slots - 1)
        at = pos
        for o, off in enumerate(offsets):
            at = jnp.where(owner[s] == away(total - off), o * slots + pos, at)
        box.append(at)
        local.append(owner[s] == me)

    settle(carried(inbox1), recv_sem.at[0])
    other = partners(turned1, inbox1)
    jump1 = [jnp.where(linked[s], weight * (other[s] - lines[s]), 0.0) for s in range(sides)]
    spread(jump1)
    add_rows(rate1, jump1)
    add_columns(rate1)

    derive(rate1)

    settle(gather, recv_sem.at[1])
    settle(corners.at[pl.ds(1, len(reach) - 1)], recv_sem.at[2])

    def whole(value):
        return jnp.broadcast_to(value, (ROWS, n))

    table = jnp.zeros((ROWS, n), jnp.float32)
    for j in range(len(reach)):
        index = (lane - j * sides + row * sides) & (n - 1)
        laid = jnp.take_along_axis(whole(corners[j]), index, axis=1)
        table = jnp.where((lane >= j * sides) & (lane < (j + 1) * sides), laid, table)
    their_owner = jnp.full((ROWS, n), -1, jnp.int32)
    their_strip = jnp.zeros((ROWS, n), jnp.int32)
    their_flip = jnp.zeros((ROWS, n), jnp.int32)
    for s in range(sides):
        here = lax.shift_right_logical(lane, 1) == s
        their_owner = jnp.where(here, owner[s], their_owner)
        their_strip = jnp.where(here, strip[s], their_strip)
        their_flip = jnp.where(here, flip[s], their_flip)

    def seat(device):
        at = jnp.zeros((ROWS, n), jnp.int32)
        for j, off in enumerate(reach):
            at = jnp.where(device == away(off), j * sides, at)
        return at

    def nook(strip, end):
        b = strip & 1
        across = (strip & 2) == 0
        return (strip & ~3) + jnp.where(across, 2 * b + 1 - end, 2 * end + 1 - b)

    end = (1 - (lane & 1)) ^ (their_flip & 1)
    base = seat(their_owner)
    beside = (their_strip & ~3) + jnp.where((their_strip & 2) == 0, 2 + end, end)
    entry = jnp.take_along_axis(table, base + beside, axis=1)
    own = jnp.take_along_axis(table, base + nook(their_strip, end), axis=1)
    far_owner = whole(entry[comps : comps + 1]).astype(jnp.int32)
    far_strip = whole(entry[comps + 1 : comps + 2]).astype(jnp.int32)
    far_flip = whole(entry[comps + 2 : comps + 3]).astype(jnp.int32)
    far_strip = jnp.where(far_owner >= 0, far_strip, 0)
    far_end = (their_strip & 1) ^ (far_flip & 1)
    value = jnp.take_along_axis(table, seat(far_owner) + nook(far_strip, far_end), axis=1)
    bend = jnp.where((far_owner >= 0) & used, weight * (value - own), 0.0)

    rest = []
    for p in range(slots):
        west, east, south, north = jump1[p * 4 : p * 4 + 4]
        mixed = (
            jnp.where(low, south, 0.0) + jnp.where(high, pltpu.roll(north, n - 1, 1), 0.0),
            jnp.where(low, pltpu.roll(south, 1, 1), 0.0) + jnp.where(high, north, 0.0),
            jnp.where(low, west, 0.0) + jnp.where(high, pltpu.roll(east, n - 1, 1), 0.0),
            jnp.where(low, pltpu.roll(west, 1, 1), 0.0) + jnp.where(high, east, 0.0),
        )
        for side in range(4):
            s = p * 4 + side
            theirs = jnp.where(edge, pltpu.roll(bend, n - (2 * s + 1), 1), 0.0)
            rest.append(theirs - mixed[side] - 2.0 * jump1[s] - lines2[s])

    best = mine[...]
    for d in range(total - 1):
        best = jnp.maximum(best, gather[d])
    bound = jnp.max(best, axis=1, keepdims=True)
    step = jnp.broadcast_to(cfl_number / (bound * (n - 1)), (ROWS, n))
    half = 0.5 * step * step

    def keep2(f, p, rows, second):
        value = fld[f, p, rows, :] + step * rate1[f, p, rows, :] + half * second
        out_v[f, p, rows, :] = jnp.where(count[0] > p, value, 0.0)

    interior(keep2)

    settle(carried(inbox2), recv_sem.at[3])
    other = partners(turned2, inbox2)
    jump2 = [
        jnp.where(linked[s], (half * weight) * (other[s] + rest[s]), 0.0) for s in range(sides)
    ]
    spread(jump2)
    add_rows(out_v, jump2)
    add_columns(out_v)

    settle(carried(outbox1), send_sem.at[0])
    settle(gather, send_sem.at[1])
    settle(corners.at[pl.ds(1, len(reach) - 1)], send_sem.at[2])
    settle(carried(outbox2), send_sem.at[3])


def shards(
    total, subs, fields, density, moduli, metric_diag, metric_cross, extension, count, connectivity
):
    comps, slots, n, _ = fields.shape
    inner, outer, _ = circulant(n, extension.shape[0])
    far = total // 2 + 1
    offsets = (1, total - 1, far, total - far)
    reach = [0, *offsets]
    for a in offsets:
        for b in offsets:
            if (a + b) % total not in reach:
                reach.append((a + b) % total)
    f32, i32 = jnp.float32, jnp.int32
    hbm = pl.BlockSpec(memory_space=pltpu.HBM)
    state = pltpu.VMEM(fields.shape, f32)
    square = pltpu.VMEM((n, n), f32)
    dma = pltpu.SemaphoreType.DMA
    boxed = pltpu.VMEM((len(offsets) * slots, 8, n), f32)
    strips = pltpu.VMEM((slots * 4, 8, n), f32)
    return pl.pallas_call(
        functools.partial(kernel, total, subs, offsets, reach),
        out_shape=pltpu.VMEM(fields.shape, f32),
        in_specs=[hbm] * 9,
        out_specs=pl.BlockSpec(memory_space=pltpu.VMEM),
        scratch_shapes=[
            pltpu.SMEM(connectivity.shape[::-1], i32),
            pltpu.SMEM(count.shape, i32),
            pltpu.VMEM(extension.shape[::-1], f32),
            pltpu.VMEM((2, n, n), f32),
            state,
            pltpu.VMEM((7,) + density.shape, f32),
            state, state, state,
            pltpu.VMEM((2 * n, 2 * n), jnp.bfloat16),
            pltpu.VMEM((2 * n, 2 * n), jnp.bfloat16),
            square, square, square,
            strips, strips, strips, strips,
            boxed, boxed, boxed, boxed,
            pltpu.VMEM((1, n), f32),
            pltpu.VMEM((len(reach), 1, n), f32),
            pltpu.VMEM((1, n), f32),
            pltpu.VMEM((total - 1, 1, n), f32),
            dma((6,)), dma((4,)), dma((4,)),
        ],
        compiler_params=pltpu.CompilerParams(collective_id=0, has_side_effects=True),
    )(connectivity.T, count, fields, density, moduli, metric_diag, metric_cross, extension.T,
      jnp.asarray(np.stack([inner, outer])))


def solution(mesh):
    placed = (
        P(None, ("patch", "sub"), None, None),
        P(("patch", "sub"), None, None),
        P(None, ("patch", "sub"), None, None),
        P(None, ("patch", "sub"), None, None),
        P(None, ("patch", "sub"), None, None),
        P(),
        P(("patch", "sub")),
        P(("patch", "sub"), None),
    )
    total = mesh.shape["patch"] * mesh.shape["sub"]
    return jax.shard_map(
        functools.partial(shards, total, mesh.shape["sub"]),
        mesh=mesh,
        in_specs=placed,
        out_specs=P(None, ("patch", "sub"), None, None),
        check_vma=False,
    )
```

```python
import functools

import jax
import jax.numpy as jnp
import numpy as np
from jax import lax
from jax.experimental import pallas as pl
from jax.experimental.pallas import tpu as pltpu
from jax.sharding import PartitionSpec as P

MESH = pl.DeviceIdType.MESH
ROWS = 8
cfl_number = 0.5
penalty_weight = 0.5


def circulant(points, extra):
    length = points + extra
    half = (length - 1) // 2
    waves = np.arange(1, half + 1, dtype=np.float64)
    weights = waves * (2.0 * np.pi * (points - 1) / length)
    shifts = np.arange(length)
    phase = 2.0 * np.pi / length * (waves[:, None] * shifts[None, :] % length)
    kernel = -(2.0 / length) * np.sum(weights[:, None] * np.sin(phase), axis=0)
    at = (np.arange(points)[:, None] - np.arange(length)[None, :]) % length
    full = kernel[at].astype(np.float32)
    padded = -(-extra // ROWS) * ROWS
    outer = np.zeros((padded, points), np.float32)
    outer[:extra] = full[:, points:].T
    return np.concatenate([full[:, :points].T, outer])


def split(x):
    hi = x.astype(jnp.bfloat16)
    lo = (x - hi.astype(jnp.float32)).astype(jnp.bfloat16)
    return hi, lo


def kernel(
    total, subs, offsets, reach,
    conn_hbm, count_hbm, fields_hbm, density_hbm, moduli_hbm, diag_hbm, cross_hbm,
    ext_hbm, consts_hbm,
    out_v,
    conn, count, ext, consts,
    fld, med, rate1, dxi, deta, left, right, ext_v, cols, trans,
    lines, lines2, turned1, turned2, outbox1, outbox2, inbox1, inbox2,
    mine, gather,
    load_sem, send_sem, recv_sem,
):
    comps, slots, n, _ = fld.shape
    sides = slots * 4
    chunks = n // ROWS
    patch, core = lax.axis_index("patch"), lax.axis_index("sub")
    me = patch * subs + core
    simple = total & (total - 1) == 0 and subs & (subs - 1) == 0
    unroll = total - 1 if total <= 64 else 1

    def away(off):
        return lax.rem(me + off, total)

    def place(flat):
        return (lax.div(flat, subs), lax.rem(flat, subs))

    def peer(d):
        if simple:
            return (patch ^ lax.div(d, subs), core ^ lax.rem(d, subs))
        return place(away(d))

    conn_load = pltpu.make_async_copy(conn_hbm, conn, load_sem.at[0])
    count_load = pltpu.make_async_copy(count_hbm, count, load_sem.at[1])
    ext_load = pltpu.make_async_copy(ext_hbm, ext, load_sem.at[2])
    consts_load = pltpu.make_async_copy(consts_hbm, consts, load_sem.at[3])
    fields_load = pltpu.make_async_copy(fields_hbm, fld, load_sem.at[4])
    med_load = pltpu.make_async_copy(med, med, load_sem.at[5])
    conn_load.start()
    for f in range(comps):
        pltpu.make_async_copy(fields_hbm.at[f], fld.at[f], load_sem.at[4]).start()
    ext_load.start()
    consts_load.start()

    barrier = pltpu.get_barrier_semaphore()

    def greet(i, _):
        pl.semaphore_signal(
            barrier, inc=1, device_id=peer(total - 1 - i), device_id_type=MESH
        )
        return _

    lax.fori_loop(0, total - 1, greet, 0, unroll=unroll)
    pltpu.make_async_copy(density_hbm, med.at[0], load_sem.at[5]).start()
    for k in range(2):
        pltpu.make_async_copy(moduli_hbm.at[k], med.at[1 + k], load_sem.at[5]).start()
        pltpu.make_async_copy(diag_hbm.at[k], med.at[3 + k], load_sem.at[5]).start()
        pltpu.make_async_copy(cross_hbm.at[k], med.at[5 + k], load_sem.at[5]).start()
    count_load.start()

    lines[...] = jnp.zeros_like(lines)
    lines2[...] = jnp.zeros_like(lines2)
    trans[...] = jnp.zeros_like(trans)
    ext_v[...] = jnp.zeros_like(ext_v)

    conn_load.wait()
    near = [away(off) for off in offsets]
    owner = [conn[0, s] for s in range(sides)]
    linked = [owner[s] >= 0 for s in range(sides)]
    strip = [jnp.where(linked[s], conn[1, s], 0) for s in range(sides)]
    flip = [conn[2, s] for s in range(sides)]
    tags = []
    for s in range(sides):
        rank = jnp.int32(0)
        for t in range(s):
            rank = rank + (owner[t] == owner[s]).astype(jnp.int32)
        tags.append(owner[s] * sides + rank)
    picks = []
    for there in near:
        pick = []
        for k in range(slots):
            tag, at = there * sides + k, jnp.int32(0)
            for s in range(1, sides):
                at = jnp.where(tags[s] == tag, s, at)
            pick.append(at)
        picks.append(pick)

    lane = lax.broadcasted_iota(jnp.int32, (ROWS, n), 1)
    row = lax.broadcasted_iota(jnp.int32, (ROWS, n), 0)
    low, high = lane == 0, lane == n - 1
    edge = low | high
    used = row < comps
    upper = lane >= n // 2
    pairs = [(f, p, p * 8 + f) for p in range(slots) for f in range(comps)]
    weight = penalty_weight * (n - 1)

    def collect(state, lines):
        def columns(c, _):
            rows = pl.ds(pl.multiple_of(c * ROWS, ROWS), ROWS)
            acc = jnp.zeros((ROWS, n), jnp.float32)
            for f, p, m in pairs:
                turned = pltpu.roll(state[f, p, rows, :], 2 * m + 1, 1)
                acc = jnp.where((lane == 2 * m) | (lane == 2 * m + 1), turned, acc)
            cols[rows, :] = acc
            return _

        lax.fori_loop(0, chunks, columns, 0, unroll=chunks)
        trans[...] = jnp.transpose(cols[...])
        for p in range(slots):
            lines[p * 4 + 2] = trans[pl.ds(p * 16 + 1, 8, stride=2), :]
            lines[p * 4 + 3] = trans[pl.ds(p * 16, 8, stride=2), :]
            for f in range(comps):
                lines[p * 4, pl.ds(f, 1)] = state[f, p, pl.ds(0, 1), :]
                lines[p * 4 + 1, pl.ds(f, 1)] = state[f, p, pl.ds(n - 1, 1), :]

    def turn(lines, turned):
        for s in range(sides):
            index = jnp.where(flip[s] == 1, n - 1 - lane, lane)
            turned[s] = jnp.take_along_axis(lines[s], index, axis=1)

    def post(turned, outbox, inbox, at, rider=None):
        for o in range(len(offsets)):
            for k in range(slots):
                line = turned[picks[o][k]]
                if rider is not None:
                    line = jnp.where(row == comps, rider, line)
                outbox[o * slots + k] = line
        height = comps + (rider is not None)
        for o in range(len(offsets)):
            spot = (pl.ds(o * slots, slots), pl.ds(0, height), slice(None))
            pltpu.make_async_remote_copy(
                src_ref=outbox.at[spot],
                dst_ref=inbox.at[spot],
                send_sem=send_sem.at[at],
                recv_sem=recv_sem.at[at],
                device_id=place(near[o]),
                device_id_type=MESH,
            ).start()

    def settle(buffer, sem):
        pltpu.make_async_copy(buffer, buffer, sem).wait()

    def carried(buffer, height):
        return buffer.at[:, pl.ds(0, height), :]

    def whole(value):
        return jnp.broadcast_to(value, (ROWS, n))

    def partners(turned, inbox):
        return [
            jnp.where(used, jnp.where(local[s], turned[strip[s]], inbox[box[s]]), 0.0)
            for s in range(sides)
        ]

    def spread(jump):
        for p in range(slots):
            trans[pl.ds(p * 16 + 1, 8, stride=2), :] = jump[p * 4 + 2]
            trans[pl.ds(p * 16, 8, stride=2), :] = jump[p * 4 + 3]
        cols[...] = jnp.transpose(trans[...])

    def derive(state):
        for f in range(comps):
            h0, l0 = split(state[f, 0])
            h1, l1 = split(state[f, 1])
            rows = jnp.concatenate(
                [jnp.concatenate([h0, l0], axis=1), jnp.concatenate([h1, l1], axis=1)], axis=0
            )
            eta = jnp.dot(rows, right[...], preferred_element_type=jnp.float32)
            both = eta[:, :n] + eta[:, n:]
            deta[f, 0] = both[:n]
            deta[f, 1] = both[n:]
            body = jnp.concatenate(
                [jnp.concatenate([h0, h1], axis=1), jnp.concatenate([l0, l1], axis=1)], axis=0
            )
            xi = jnp.dot(left[...], body, preferred_element_type=jnp.float32)
            both = xi[:n] + xi[n:]
            dxi[f, 0] = both[:, :n]
            dxi[f, 1] = both[:, n:]

    def interior(keep):
        for p in range(slots):

            def body(c, _):
                rows = pl.ds(pl.multiple_of(c * ROWS, ROWS), ROWS)
                inv, lame, shear, xx, yy, xy, ex = (med[k, p, rows, :] for k in range(7))
                stiff = lame + 2.0 * shear
                ax = [dxi[f, p, rows, :] for f in range(comps)]
                ay = [deta[f, p, rows, :] for f in range(comps)]
                gx = [xx * a + ex * b for a, b in zip(ax, ay)]
                gy = [xy * a + yy * b for a, b in zip(ax, ay)]
                keep(0, p, rows, (gx[2] + gy[4]) * inv)
                keep(1, p, rows, (gx[4] + gy[3]) * inv)
                keep(2, p, rows, stiff * gx[0] + lame * gy[1])
                keep(3, p, rows, lame * gx[0] + stiff * gy[1])
                keep(4, p, rows, shear * (gy[0] + gx[1]))
                return _

            lax.fori_loop(0, chunks, body, 0, unroll=chunks)

    def add_rows(state, jump):
        for p in range(slots):
            for f in range(comps):
                for side, at in ((0, 0), (1, n - 1)):
                    spot = pl.ds(at, 1)
                    state[f, p, spot, :] = state[f, p, spot, :] + jump[p * 4 + side][f : f + 1]

    def add_columns(state):
        def body(c, _):
            rows = pl.ds(pl.multiple_of(c * ROWS, ROWS), ROWS)
            both = cols[rows, :]
            for f, p, m in pairs:
                side = pltpu.roll(both, n - (2 * m + 1), 1)
                state[f, p, rows, :] = state[f, p, rows, :] + jnp.where(edge, side, 0.0)
            return _

        lax.fori_loop(0, chunks, body, 0, unroll=chunks)

    fields_load.wait()
    ext_load.wait()
    consts_load.wait()
    twice, extra = ext.shape
    edges = twice // 2
    ext_v[pl.ds(0, twice), pl.ds(0, extra)] = ext[...]
    bent = jnp.dot(
        ext_v[...],
        consts[pl.ds(n, ext_v.shape[1]), :],
        precision=lax.Precision.HIGHEST,
        preferred_element_type=jnp.float32,
    )
    consts[pl.ds(n - edges, edges), :] = consts[pl.ds(n - edges, edges), :] + bent[:edges]
    consts[pl.ds(0, edges), :] = consts[pl.ds(0, edges), :] + bent[edges:twice]
    matrix = consts[pl.ds(0, n), :]
    hi, lo = split(matrix)
    none = jnp.zeros_like(hi)
    right[...] = jnp.concatenate(
        [jnp.concatenate([hi, lo], axis=1), jnp.concatenate([hi, none], axis=1)], axis=0
    )
    hi, lo = split(jnp.transpose(matrix))
    left[...] = jnp.concatenate(
        [jnp.concatenate([hi, hi], axis=1), jnp.concatenate([lo, none], axis=1)], axis=0
    )
    collect(fld, lines)
    turn(lines, turned1)
    table = jnp.zeros((ROWS, n), jnp.int32)
    for r in range(3):
        for s in range(sides):
            table = jnp.where(lane == r * sides + s, conn[r, s], table)
    table = table.astype(jnp.float32)

    pl.semaphore_wait(barrier, total - 1)
    post(turned1, outbox1, inbox1, 0, table)

    count_load.wait()
    med_load.wait()
    tile = jnp.zeros((ROWS, n), jnp.float32)
    for p in range(slots):
        for b in range(2):
            first = p * 4 + 2 * b
            rolled = pltpu.roll(lines[p * 4 + b], first + 1, 1)
            tile = jnp.where((lane == first) | (lane == first + 1), rolled, tile)
    tile = pltpu.roll(jnp.where(used, tile, 0.0), 0, 1, stride=sides, stride_axis=0)
    packed = jnp.sum(tile, axis=0, keepdims=True)

    top = jnp.zeros((ROWS, n), jnp.float32)
    for p in range(slots):

        def speeds(c, top):
            rows = pl.ds(pl.multiple_of(c * ROWS, ROWS), ROWS)
            dens, lame, shear, xx, yy, xy, ex = (med[k, p, rows, :] for k in range(7))
            inv = 1.0 / dens
            med[0, p, rows, :] = inv
            speed = jnp.sqrt((lame + 2.0 * shear) * inv) * (
                jnp.sqrt(xx * xx + xy * xy) + jnp.sqrt(ex * ex + yy * yy)
            )
            return jnp.maximum(top, speed)

        part = lax.fori_loop(
            0, chunks, speeds, jnp.zeros((ROWS, n), jnp.float32), unroll=chunks
        )
        top = jnp.maximum(top, jnp.where(count[0] > p, part, 0.0))
    top = jnp.max(jnp.maximum(top, pltpu.roll(top, n // 2, 1)), axis=0, keepdims=True)
    mine[...] = jnp.where(upper[:1], top, packed)
    derive(fld)

    def tell(i, _):
        d = total - 1 - i
        pltpu.make_async_remote_copy(
            src_ref=mine,
            dst_ref=gather.at[d - 1],
            send_sem=send_sem.at[1],
            recv_sem=recv_sem.at[1],
            device_id=peer(d),
            device_id_type=MESH,
        ).start()
        return _

    lax.fori_loop(0, total - 1, tell, 0, unroll=unroll)

    def keep1(f, p, rows, value):
        rate1[f, p, rows, :] = value

    interior(keep1)
    collect(rate1, lines2)
    turn(lines2, turned2)
    post(turned2, outbox2, inbox2, 2)

    box, local = [], []
    for s in range(sides):
        pos = jnp.int32(0)
        for t in range(sides):
            if t != s:
                pos = pos + ((owner[t] == owner[s]) & (strip[t] < strip[s])).astype(jnp.int32)
        pos = jnp.minimum(pos, slots - 1)
        at = pos
        for o, off in enumerate(offsets):
            at = jnp.where(owner[s] == away(total - off), o * slots + pos, at)
        box.append(at)
        local.append(owner[s] == me)

    settle(carried(inbox1, comps + 1), recv_sem.at[0])
    other = partners(turned1, inbox1)
    jump1 = [jnp.where(linked[s], weight * (other[s] - lines[s]), 0.0) for s in range(sides)]
    spread(jump1)
    add_rows(rate1, jump1)
    add_columns(rate1)
    derive(rate1)

    def keep2(f, p, rows, value):
        out_v[f, p, rows, :] = value

    interior(keep2)

    their_owner = jnp.full((ROWS, n), -1, jnp.int32)
    their_strip = jnp.zeros((ROWS, n), jnp.int32)
    their_flip = jnp.zeros((ROWS, n), jnp.int32)
    for s in range(sides):
        here = lax.shift_right_logical(lane, 1) == s
        their_owner = jnp.where(here, owner[s], their_owner)
        their_strip = jnp.where(here, strip[s], their_strip)
        their_flip = jnp.where(here, flip[s], their_flip)

    def seat(device, count):
        at = jnp.zeros((ROWS, n), jnp.int32)
        for j in range(1, count):
            at = jnp.where(device == away(reach[j]), j, at)
        return at

    def nook(strip, end):
        b = strip & 1
        across = (strip & 2) == 0
        return (strip & ~3) + jnp.where(across, 2 * b + 1 - end, 2 * end + 1 - b)

    def look(rows, seats, index):
        found = jnp.zeros((ROWS, n), jnp.float32)
        index = row * sides + index
        for j, line in enumerate(rows):
            found = jnp.where(seats == j, jnp.take_along_axis(line, index, axis=1), found)
        return found

    close = 1 + len(offsets)
    tables = [table]
    for j in range(1, close):
        o = offsets.index(total - reach[j])
        tables.append(whole(inbox1[o * slots, pl.ds(comps, 1), :]))
    end = (1 - (lane & 1)) ^ (their_flip & 1)
    base = seat(their_owner, close)
    beside = (their_strip & ~3) + jnp.where((their_strip & 2) == 0, 2 + end, end)
    entry = look(tables, base, beside)
    far_owner, far_strip, far_flip = (whole(entry[r : r + 1]).astype(jnp.int32) for r in range(3))
    far_strip = jnp.where(far_owner >= 0, far_strip, 0)
    far_end = (their_strip & 1) ^ (far_flip & 1)
    far_seat = seat(far_owner, len(reach))
    far_nook = nook(far_strip, far_end)
    near_nook = nook(their_strip, end)

    rest = []
    for p in range(slots):
        west, east, south, north = jump1[p * 4 : p * 4 + 4]
        mixed = (
            jnp.where(low, south, 0.0) + jnp.where(high, pltpu.roll(north, n - 1, 1), 0.0),
            jnp.where(low, pltpu.roll(south, 1, 1), 0.0) + jnp.where(high, north, 0.0),
            jnp.where(low, west, 0.0) + jnp.where(high, pltpu.roll(east, n - 1, 1), 0.0),
            jnp.where(low, pltpu.roll(west, 1, 1), 0.0) + jnp.where(high, east, 0.0),
        )
        for side in range(4):
            s = p * 4 + side
            rest.append(-mixed[side] - 2.0 * jump1[s] - lines2[s])

    settle(gather, recv_sem.at[1])

    def report(off):
        if simple:
            return gather[(me ^ away(off)) - 1]
        return gather[total - off - 1]

    reports = [whole(mine[...])] + [whole(report(off)) for off in reach[1:]]
    value = look(reports, far_seat, far_nook)
    own = look(reports[:close], base, near_nook)
    bend = jnp.where((far_owner >= 0) & used, weight * (value - own), 0.0)
    best = [mine[...]] + [gather[d] for d in range(total - 1)]
    while len(best) > 1:
        best = [jnp.maximum(*best[k : k + 2]) if k + 1 < len(best) else best[k]
                for k in range(0, len(best), 2)]
    bound = jnp.max(jnp.where(upper[:1], best[0], 0.0), axis=1, keepdims=True)
    step = jnp.broadcast_to(cfl_number / (bound * (n - 1)), (ROWS, n))
    half = 0.5 * step * step
    for p in range(slots):

        def settled(c, _):
            rows = pl.ds(pl.multiple_of(c * ROWS, ROWS), ROWS)
            for f in range(comps):
                value = fld[f, p, rows, :] + step * rate1[f, p, rows, :]
                value = value + half * out_v[f, p, rows, :]
                out_v[f, p, rows, :] = jnp.where(count[0] > p, value, 0.0)
            return _

        lax.fori_loop(0, chunks, settled, 0, unroll=chunks)
    for s in range(sides):
        rest[s] = rest[s] + jnp.where(edge, pltpu.roll(bend, n - (2 * s + 1), 1), 0.0)

    settle(carried(inbox2, comps), recv_sem.at[2])
    other = partners(turned2, inbox2)
    jump2 = [
        jnp.where(linked[s], (half * weight) * (other[s] + rest[s]), 0.0) for s in range(sides)
    ]
    spread(jump2)
    add_rows(out_v, jump2)
    add_columns(out_v)

    settle(carried(outbox1, comps + 1), send_sem.at[0])
    settle(gather, send_sem.at[1])
    settle(carried(outbox2, comps), send_sem.at[2])


def shards(
    total, subs, fields, density, moduli, metric_diag, metric_cross, extension, count, connectivity
):
    comps, slots, n, _ = fields.shape
    consts = circulant(n, extension.shape[0])
    far = total // 2 + 1
    offsets = (1, total - 1, far, total - far)
    reach = [0, *offsets]
    for a in offsets:
        for b in offsets:
            if (a + b) % total not in reach:
                reach.append((a + b) % total)
    f32, i32 = jnp.float32, jnp.int32
    hbm = pl.BlockSpec(memory_space=pltpu.HBM)
    state = pltpu.VMEM(fields.shape, f32)
    square = pltpu.VMEM((n, n), f32)
    dma = pltpu.SemaphoreType.DMA
    boxed = pltpu.VMEM((len(offsets) * slots, 8, n), f32)
    strips = pltpu.VMEM((slots * 4, 8, n), f32)
    return pl.pallas_call(
        functools.partial(kernel, total, subs, offsets, reach),
        out_shape=pltpu.VMEM(fields.shape, f32),
        in_specs=[hbm] * 9,
        out_specs=pl.BlockSpec(memory_space=pltpu.VMEM),
        scratch_shapes=[
            pltpu.SMEM(connectivity.shape[::-1], i32),
            pltpu.SMEM(count.shape, i32),
            pltpu.VMEM(extension.shape[::-1], f32),
            pltpu.VMEM(consts.shape, f32),
            state,
            pltpu.VMEM((7,) + density.shape, f32),
            state, state, state,
            pltpu.VMEM((2 * n, 2 * n), jnp.bfloat16),
            pltpu.VMEM((2 * n, 2 * n), jnp.bfloat16),
            pltpu.VMEM((-(-extension.shape[1] // ROWS) * ROWS, consts.shape[0] - n), f32),
            square, square,
            strips, strips, strips, strips,
            boxed, boxed, boxed, boxed,
            pltpu.VMEM((1, n), f32),
            pltpu.VMEM((total - 1, 1, n), f32),
            dma((6,)), dma((3,)), dma((3,)),
        ],
        compiler_params=pltpu.CompilerParams(collective_id=0, has_side_effects=True),
    )(connectivity.T, count, fields, density, moduli, metric_diag, metric_cross, extension.T,
      jnp.asarray(consts))


def solution(mesh):
    placed = (
        P(None, ("patch", "sub"), None, None),
        P(("patch", "sub"), None, None),
        P(None, ("patch", "sub"), None, None),
        P(None, ("patch", "sub"), None, None),
        P(None, ("patch", "sub"), None, None),
        P(),
        P(("patch", "sub")),
        P(("patch", "sub"), None),
    )
    total = mesh.shape["patch"] * mesh.shape["sub"]
    return jax.shard_map(
        functools.partial(shards, total, mesh.shape["sub"]),
        mesh=mesh,
        in_specs=placed,
        out_specs=P(None, ("patch", "sub"), None, None),
        check_vma=False,
    )
```

```python
import functools

import jax
import jax.numpy as jnp
import numpy as np
from jax import lax
from jax.experimental import pallas as pl
from jax.experimental.pallas import tpu as pltpu
from jax.sharding import PartitionSpec as P

LOGICAL = pl.DeviceIdType.LOGICAL
ROWS = 8
cfl_number = 0.5
penalty_weight = 0.5


def circulant(points, extra):
    length = points + extra
    half = (length - 1) // 2
    waves = np.arange(1, half + 1, dtype=np.float64)
    weights = waves * (2.0 * np.pi * (points - 1) / length)
    shifts = np.arange(length)
    phase = 2.0 * np.pi / length * (waves[:, None] * shifts[None, :] % length)
    kernel = -(2.0 / length) * np.sum(weights[:, None] * np.sin(phase), axis=0)
    at = (np.arange(points)[:, None] - np.arange(length)[None, :]) % length
    full = kernel[at].astype(np.float32)
    padded = -(-extra // ROWS) * ROWS
    outer = np.zeros((padded, points), np.float32)
    outer[:extra] = full[:, points:].T
    return np.concatenate([full[:, :points].T, outer])


def split(x):
    hi = x.astype(jnp.bfloat16)
    lo = (x - hi.astype(jnp.float32)).astype(jnp.bfloat16)
    return hi, lo


def kernel(
    total, subs, offsets, reach,
    conn_hbm, count_hbm, fields_hbm, density_hbm, moduli_hbm, diag_hbm, cross_hbm,
    ext_hbm, consts_hbm,
    fld, rate1, rate2, cols, edges2, factors,
    conn, count, ext, consts,
    med, dxi, deta, left, right, ext_v, trans,
    lines, lines2, turned1, turned2, outbox1, outbox2, inbox1, inbox2,
    mine, gather,
    load_sem, send_sem, recv_sem,
):
    comps, slots, n, _ = fld.shape
    sides = slots * 4
    chunks = n // ROWS
    me = lax.axis_index("patch") * subs + lax.axis_index("sub")
    simple = total & (total - 1) == 0
    unroll = total - 1 if total <= 64 else 1

    def away(off):
        return lax.rem(me + off, total)

    def peer(d):
        return me ^ d if simple else away(d)

    conn_load = pltpu.make_async_copy(conn_hbm, conn, load_sem.at[0])
    count_load = pltpu.make_async_copy(count_hbm, count, load_sem.at[1])
    ext_load = pltpu.make_async_copy(ext_hbm, ext, load_sem.at[2])
    consts_load = pltpu.make_async_copy(consts_hbm, consts, load_sem.at[3])
    fields_load = pltpu.make_async_copy(fields_hbm, fld, load_sem.at[4])
    med_load = pltpu.make_async_copy(med, med, load_sem.at[5])
    conn_load.start()
    ext_load.start()
    tall = consts.shape[0] // 5
    for k in range(5):
        part = pl.ds(k * tall, tall)
        pltpu.make_async_copy(consts_hbm.at[part], consts.at[part], load_sem.at[3]).start()

    def fetch(src, dst, sem, cuts):
        for p in range(slots):
            for k in range(cuts):
                part = (p, pl.ds(k * (n // cuts), n // cuts))
                pltpu.make_async_copy(src.at[part], dst.at[part], sem).start()

    for f in range(comps):
        fetch(fields_hbm.at[f], fld.at[f], load_sem.at[4], 4)
    count_load.start()
    fetch(density_hbm, med.at[0], load_sem.at[5], 2)
    for k in range(2):
        fetch(moduli_hbm.at[k], med.at[1 + k], load_sem.at[5], 2)
    for k in range(2):
        fetch(diag_hbm.at[k], med.at[3 + k], load_sem.at[5], 2)
        fetch(cross_hbm.at[k], med.at[5 + k], load_sem.at[5], 2)

    barrier = pltpu.get_barrier_semaphore()

    def greet(i, _):
        pl.semaphore_signal(
            barrier, inc=1, device_id=peer(total - 1 - i), device_id_type=LOGICAL
        )
        return _

    lax.fori_loop(0, total - 1, greet, 0, unroll=unroll)
    lines[...] = jnp.zeros_like(lines)
    lines2[...] = jnp.zeros_like(lines2)
    trans[...] = jnp.zeros_like(trans)
    ext_v[...] = jnp.zeros_like(ext_v)

    conn_load.wait()
    near = [away(off) for off in offsets]
    owner = [conn[0, s] for s in range(sides)]
    linked = [owner[s] >= 0 for s in range(sides)]
    strip = [jnp.where(linked[s], conn[1, s], 0) for s in range(sides)]
    flip = [conn[2, s] for s in range(sides)]
    tags = []
    for s in range(sides):
        rank = jnp.int32(0)
        for t in range(s):
            rank = rank + (owner[t] == owner[s]).astype(jnp.int32)
        tags.append(owner[s] * sides + rank)
    picks = []
    for there in near:
        pick = []
        for k in range(slots):
            tag, at = there * sides + k, jnp.int32(0)
            for s in range(1, sides):
                at = jnp.where(tags[s] == tag, s, at)
            pick.append(at)
        picks.append(pick)

    lane = lax.broadcasted_iota(jnp.int32, (ROWS, n), 1)
    row = lax.broadcasted_iota(jnp.int32, (ROWS, n), 0)
    low, high = lane == 0, lane == n - 1
    edge = low | high
    used = row < comps
    pairs = [(f, p, p * 8 + f) for p in range(slots) for f in range(comps)]
    weight = penalty_weight * (n - 1)

    def collect(state, lines):
        def columns(c, _):
            rows = pl.ds(pl.multiple_of(c * ROWS, ROWS), ROWS)
            acc = jnp.zeros((ROWS, n), jnp.float32)
            for f, p, m in pairs:
                turned = pltpu.roll(state[f, p, rows, :], 2 * m + 1, 1)
                acc = jnp.where((lane == 2 * m) | (lane == 2 * m + 1), turned, acc)
            cols[rows, :] = acc
            return _

        lax.fori_loop(0, chunks, columns, 0, unroll=chunks)
        trans[...] = jnp.transpose(cols[...])
        for p in range(slots):
            lines[p * 4 + 2] = trans[pl.ds(p * 16 + 1, 8, stride=2), :]
            lines[p * 4 + 3] = trans[pl.ds(p * 16, 8, stride=2), :]
            for f in range(comps):
                lines[p * 4, pl.ds(f, 1)] = state[f, p, pl.ds(0, 1), :]
                lines[p * 4 + 1, pl.ds(f, 1)] = state[f, p, pl.ds(n - 1, 1), :]

    def turn(lines, turned):
        for s in range(sides):
            index = jnp.where(flip[s] == 1, n - 1 - lane, lane)
            turned[s] = jnp.take_along_axis(lines[s], index, axis=1)

    def post(turned, outbox, inbox, at, rider=None):
        for o in range(len(offsets)):
            for k in range(slots):
                line = turned[picks[o][k]]
                if rider is not None:
                    line = jnp.where(row == comps, rider, line)
                outbox[o * slots + k] = line
        height = comps + (rider is not None)
        for o in range(len(offsets)):
            spot = (pl.ds(o * slots, slots), pl.ds(0, height), slice(None))
            pltpu.make_async_remote_copy(
                src_ref=outbox.at[spot],
                dst_ref=inbox.at[spot],
                send_sem=send_sem.at[at],
                recv_sem=recv_sem.at[at],
                device_id=near[o],
                device_id_type=LOGICAL,
            ).start()

    def settle(buffer, sem):
        pltpu.make_async_copy(buffer, buffer, sem).wait()

    def carried(buffer, height):
        return buffer.at[:, pl.ds(0, height), :]

    def whole(value):
        return jnp.broadcast_to(value, (ROWS, n))

    def partners(turned, inbox):
        return [
            jnp.where(used, jnp.where(local[s], turned[strip[s]], inbox[box[s]]), 0.0)
            for s in range(sides)
        ]

    def spread(jump):
        for p in range(slots):
            trans[pl.ds(p * 16 + 1, 8, stride=2), :] = jump[p * 4 + 2]
            trans[pl.ds(p * 16, 8, stride=2), :] = jump[p * 4 + 3]
        cols[...] = jnp.transpose(trans[...])

    def derive(state):
        for f in range(comps):
            h0, l0 = split(state[f, 0])
            h1, l1 = split(state[f, 1])
            rows = jnp.concatenate(
                [jnp.concatenate([h0, l0], axis=1), jnp.concatenate([h1, l1], axis=1)], axis=0
            )
            eta = jnp.dot(rows, right[...], preferred_element_type=jnp.float32)
            both = eta[:, :n] + eta[:, n:]
            deta[f, 0] = both[:n]
            deta[f, 1] = both[n:]
            body = jnp.concatenate(
                [jnp.concatenate([h0, h1], axis=1), jnp.concatenate([l0, l1], axis=1)], axis=0
            )
            xi = jnp.dot(left[...], body, preferred_element_type=jnp.float32)
            both = xi[:n] + xi[n:]
            dxi[f, 0] = both[:, :n]
            dxi[f, 1] = both[:, n:]

    def interior(keep):
        for p in range(slots):

            def body(c, _):
                rows = pl.ds(pl.multiple_of(c * ROWS, ROWS), ROWS)
                inv, lame, shear, xx, yy, xy, ex = (med[k, p, rows, :] for k in range(7))
                stiff = lame + 2.0 * shear
                ax = [dxi[f, p, rows, :] for f in range(comps)]
                ay = [deta[f, p, rows, :] for f in range(comps)]
                gx = [xx * a + ex * b for a, b in zip(ax, ay)]
                gy = [xy * a + yy * b for a, b in zip(ax, ay)]
                keep(0, p, rows, (gx[2] + gy[4]) * inv)
                keep(1, p, rows, (gx[4] + gy[3]) * inv)
                keep(2, p, rows, stiff * gx[0] + lame * gy[1])
                keep(3, p, rows, lame * gx[0] + stiff * gy[1])
                keep(4, p, rows, shear * (gy[0] + gx[1]))
                return _

            lax.fori_loop(0, chunks, body, 0, unroll=chunks)

    def add_rows(state, jump):
        for p in range(slots):
            for f in range(comps):
                for side, at in ((0, 0), (1, n - 1)):
                    spot = pl.ds(at, 1)
                    state[f, p, spot, :] = state[f, p, spot, :] + jump[p * 4 + side][f : f + 1]

    def add_columns(state):
        def body(c, _):
            rows = pl.ds(pl.multiple_of(c * ROWS, ROWS), ROWS)
            both = cols[rows, :]
            for f, p, m in pairs:
                side = pltpu.roll(both, n - (2 * m + 1), 1)
                state[f, p, rows, :] = state[f, p, rows, :] + jnp.where(edge, side, 0.0)
            return _

        lax.fori_loop(0, chunks, body, 0, unroll=chunks)

    fields_load.wait()
    ext_load.wait()
    consts_load.wait()
    twice, extra = ext.shape
    edges = twice // 2
    ext_v[pl.ds(0, twice), pl.ds(0, extra)] = ext[...]
    bent = jnp.dot(
        ext_v[...],
        consts[pl.ds(n, ext_v.shape[1]), :],
        precision=lax.Precision.HIGHEST,
        preferred_element_type=jnp.float32,
    )
    consts[pl.ds(n - edges, edges), :] = consts[pl.ds(n - edges, edges), :] + bent[:edges]
    consts[pl.ds(0, edges), :] = consts[pl.ds(0, edges), :] + bent[edges:twice]
    matrix = consts[pl.ds(0, n), :]
    hi, lo = split(matrix)
    none = jnp.zeros_like(hi)
    right[...] = jnp.concatenate(
        [jnp.concatenate([hi, lo], axis=1), jnp.concatenate([hi, none], axis=1)], axis=0
    )
    hi, lo = split(jnp.transpose(matrix))
    left[...] = jnp.concatenate(
        [jnp.concatenate([hi, hi], axis=1), jnp.concatenate([lo, none], axis=1)], axis=0
    )
    collect(fld, lines)
    turn(lines, turned1)
    table = jnp.zeros((ROWS, n), jnp.int32)
    for r in range(3):
        for s in range(sides):
            table = jnp.where(lane == r * sides + s, conn[r, s], table)
    table = table.astype(jnp.float32)

    pl.semaphore_wait(barrier, total - 1)
    post(turned1, outbox1, inbox1, 0, table)

    count_load.wait()
    med_load.wait()
    tile = jnp.zeros((ROWS, n), jnp.float32)
    for p in range(slots):
        for b in range(2):
            first = p * 4 + 2 * b
            rolled = pltpu.roll(lines[p * 4 + b], first + 1, 1)
            tile = jnp.where((lane == first) | (lane == first + 1), rolled, tile)
    tile = pltpu.roll(jnp.where(used, tile, 0.0), 0, 1, stride=sides, stride_axis=0)
    packed = jnp.sum(tile, axis=0, keepdims=True)

    top = jnp.zeros((ROWS, n), jnp.float32)
    for p in range(slots):

        def speeds(c, top):
            rows = pl.ds(pl.multiple_of(c * ROWS, ROWS), ROWS)
            dens, lame, shear, xx, yy, xy, ex = (med[k, p, rows, :] for k in range(7))
            inv = 1.0 / dens
            med[0, p, rows, :] = inv
            speed = jnp.sqrt((lame + 2.0 * shear) * inv) * (
                jnp.sqrt(xx * xx + xy * xy) + jnp.sqrt(ex * ex + yy * yy)
            )
            return jnp.maximum(top, speed)

        part = lax.fori_loop(
            0, chunks, speeds, jnp.zeros((ROWS, n), jnp.float32), unroll=chunks
        )
        top = jnp.maximum(top, jnp.where(count[0] > p, part, 0.0))
    mine[...] = jnp.concatenate([jnp.max(top, axis=0, keepdims=True), packed], axis=0)

    def tell(i, _):
        d = total - 1 - i
        pltpu.make_async_remote_copy(
            src_ref=mine,
            dst_ref=gather.at[d - 1],
            send_sem=send_sem.at[1],
            recv_sem=recv_sem.at[1],
            device_id=peer(d),
            device_id_type=LOGICAL,
        ).start()
        return _

    lax.fori_loop(0, total - 1, tell, 0, unroll=unroll)

    derive(fld)

    def keep1(f, p, rows, value):
        rate1[f, p, rows, :] = value

    interior(keep1)
    collect(rate1, lines2)
    turn(lines2, turned2)
    post(turned2, outbox2, inbox2, 2)

    box, local = [], []
    for s in range(sides):
        pos = jnp.int32(0)
        for t in range(sides):
            if t != s:
                pos = pos + ((owner[t] == owner[s]) & (strip[t] < strip[s])).astype(jnp.int32)
        pos = jnp.minimum(pos, slots - 1)
        at = pos
        for o, off in enumerate(offsets):
            at = jnp.where(owner[s] == away(total - off), o * slots + pos, at)
        box.append(at)
        local.append(owner[s] == me)

    settle(carried(inbox1, comps + 1), recv_sem.at[0])
    other = partners(turned1, inbox1)
    jump1 = [jnp.where(linked[s], weight * (other[s] - lines[s]), 0.0) for s in range(sides)]
    spread(jump1)
    add_rows(rate1, jump1)
    add_columns(rate1)
    derive(rate1)

    def keep2(f, p, rows, value):
        rate2[f, p, rows, :] = value

    interior(keep2)

    their_owner = jnp.full((ROWS, n), -1, jnp.int32)
    their_strip = jnp.zeros((ROWS, n), jnp.int32)
    their_flip = jnp.zeros((ROWS, n), jnp.int32)
    for s in range(sides):
        here = lax.shift_right_logical(lane, 1) == s
        their_owner = jnp.where(here, owner[s], their_owner)
        their_strip = jnp.where(here, strip[s], their_strip)
        their_flip = jnp.where(here, flip[s], their_flip)

    def seat(device, count):
        at = jnp.zeros((ROWS, n), jnp.int32)
        for j in range(1, count):
            at = jnp.where(device == away(reach[j]), j, at)
        return at

    def nook(strip, end):
        b = strip & 1
        across = (strip & 2) == 0
        return (strip & ~3) + jnp.where(across, 2 * b + 1 - end, 2 * end + 1 - b)

    def look(rows, seats, index):
        found = jnp.zeros((ROWS, n), jnp.float32)
        index = row * sides + index
        for j, line in enumerate(rows):
            found = jnp.where(seats == j, jnp.take_along_axis(line, index, axis=1), found)
        return found

    close = 1 + len(offsets)
    tables = [table]
    for j in range(1, close):
        o = offsets.index(total - reach[j])
        tables.append(whole(inbox1[o * slots, pl.ds(comps, 1), :]))
    end = (1 - (lane & 1)) ^ (their_flip & 1)
    base = seat(their_owner, close)
    beside = (their_strip & ~3) + jnp.where((their_strip & 2) == 0, 2 + end, end)
    entry = look(tables, base, beside)
    far_owner, far_strip, far_flip = (whole(entry[r : r + 1]).astype(jnp.int32) for r in range(3))
    far_strip = jnp.where(far_owner >= 0, far_strip, 0)
    far_end = (their_strip & 1) ^ (far_flip & 1)
    far_seat = seat(far_owner, len(reach))
    far_nook = nook(far_strip, far_end)
    near_nook = nook(their_strip, end)

    rest = []
    for p in range(slots):
        west, east, south, north = jump1[p * 4 : p * 4 + 4]
        mixed = (
            jnp.where(low, south, 0.0) + jnp.where(high, pltpu.roll(north, n - 1, 1), 0.0),
            jnp.where(low, pltpu.roll(south, 1, 1), 0.0) + jnp.where(high, north, 0.0),
            jnp.where(low, west, 0.0) + jnp.where(high, pltpu.roll(east, n - 1, 1), 0.0),
            jnp.where(low, pltpu.roll(west, 1, 1), 0.0) + jnp.where(high, east, 0.0),
        )
        for side in range(4):
            s = p * 4 + side
            rest.append(-mixed[side] - 2.0 * jump1[s] - lines2[s])

    settle(gather, recv_sem.at[1])

    def report(off):
        if simple:
            return gather[(me ^ away(off)) - 1, 1:]
        return gather[total - off - 1, 1:]

    reports = [whole(mine[1:])] + [whole(report(off)) for off in reach[1:]]
    value = look(reports, far_seat, far_nook)
    own = look(reports[:close], base, near_nook)
    bend = jnp.where((far_owner >= 0) & used, weight * (value - own), 0.0)
    best = [mine[:1]] + [gather[d, :1] for d in range(total - 1)]
    while len(best) > 1:
        best = [jnp.maximum(*best[k : k + 2]) if k + 1 < len(best) else best[k]
                for k in range(0, len(best), 2)]
    bound = jnp.max(best[0], axis=1, keepdims=True)
    step = jnp.broadcast_to(cfl_number / (bound * (n - 1)), (ROWS, n))
    half = 0.5 * step * step
    factors[0] = step
    factors[1] = half
    for p in range(slots):
        factors[2 + p] = jnp.where(count[0] > p, 1.0, 0.0) + jnp.zeros((ROWS, n), jnp.float32)
    for s in range(sides):
        rest[s] = rest[s] + jnp.where(edge, pltpu.roll(bend, n - (2 * s + 1), 1), 0.0)

    settle(carried(inbox2, comps), recv_sem.at[2])
    other = partners(turned2, inbox2)
    jump2 = [
        jnp.where(linked[s], (half * weight) * (other[s] + rest[s]), 0.0) for s in range(sides)
    ]
    spread(jump2)
    for s in range(sides):
        edges2[s] = jump2[s]

    settle(carried(outbox1, comps + 1), send_sem.at[0])
    settle(gather, send_sem.at[1])
    settle(carried(outbox2, comps), send_sem.at[2])


def finish(fld, rate1, rate2, cols, edges2, factors, out_hbm, out_v, sem):
    comps, slots, n, _ = fld.shape
    chunks = n // ROWS
    lane = lax.broadcasted_iota(jnp.int32, (ROWS, n), 1)
    row = lax.broadcasted_iota(jnp.int32, (ROWS, n), 0)
    edge = (lane == 0) | (lane == n - 1)
    step, half = factors[0], factors[1]
    for p in range(slots):
        live = factors[2 + p] > 0.0
        for f in range(comps):
            for c in range(chunks):
                rows = pl.ds(c * ROWS, ROWS)
                side = pltpu.roll(cols[rows, :], n - (2 * (p * 8 + f) + 1), 1)
                value = fld[f, p, rows, :] + step * rate1[f, p, rows, :]
                value = value + half * rate2[f, p, rows, :] + jnp.where(edge, side, 0.0)
                for side, at in ((0, 0), (1, chunks - 1)):
                    if c == at:
                        line = jnp.broadcast_to(edges2[p * 4 + side, pl.ds(f, 1), :], (ROWS, n))
                        value = value + jnp.where(row == side * (ROWS - 1), line, 0.0)
                out_v[f, p, rows, :] = jnp.where(live, value, 0.0)
            pltpu.make_async_copy(out_v.at[f, p], out_hbm.at[f, p], sem.at[0]).start()
    pltpu.make_async_copy(out_v, out_hbm, sem.at[0]).wait()


def shards(
    total, subs, fields, density, moduli, metric_diag, metric_cross, extension, count, connectivity
):
    comps, slots, n, _ = fields.shape
    consts = circulant(n, extension.shape[0])
    far = total // 2 + 1
    offsets = (1, total - 1, far, total - far)
    reach = [0, *offsets]
    for a in offsets:
        for b in offsets:
            if (a + b) % total not in reach:
                reach.append((a + b) % total)
    f32, i32 = jnp.float32, jnp.int32
    hbm = pl.BlockSpec(memory_space=pltpu.HBM)
    state = pltpu.VMEM(fields.shape, f32)
    square = pltpu.VMEM((n, n), f32)
    dma = pltpu.SemaphoreType.DMA
    boxed = pltpu.VMEM((len(offsets) * slots, 8, n), f32)
    strips = pltpu.VMEM((slots * 4, 8, n), f32)
    factors = pltpu.VMEM((2 + slots, ROWS, n), f32)
    vmem = pl.BlockSpec(memory_space=pltpu.VMEM)
    parts = pl.pallas_call(
        functools.partial(kernel, total, subs, offsets, reach),
        out_shape=[state, state, state, square, strips, factors],
        in_specs=[hbm] * 9,
        out_specs=[vmem] * 6,
        scratch_shapes=[
            pltpu.SMEM(connectivity.shape[::-1], i32),
            pltpu.SMEM(count.shape, i32),
            pltpu.VMEM(extension.shape[::-1], f32),
            pltpu.VMEM(consts.shape, f32),
            pltpu.VMEM((7,) + density.shape, f32),
            state, state,
            pltpu.VMEM((2 * n, 2 * n), jnp.bfloat16),
            pltpu.VMEM((2 * n, 2 * n), jnp.bfloat16),
            pltpu.VMEM((-(-extension.shape[1] // ROWS) * ROWS, consts.shape[0] - n), f32),
            square,
            strips, strips, strips, strips,
            boxed, boxed, boxed, boxed,
            pltpu.VMEM((2, n), f32),
            pltpu.VMEM((total - 1, 2, n), f32),
            dma((6,)), dma((3,)), dma((3,)),
        ],
        compiler_params=pltpu.CompilerParams(collective_id=0, has_side_effects=True),
    )(connectivity.T, count, fields, density, moduli, metric_diag, metric_cross, extension.T,
      jnp.asarray(consts))
    return pl.pallas_call(
        finish,
        out_shape=jax.ShapeDtypeStruct(fields.shape, f32),
        in_specs=[vmem] * 6,
        out_specs=hbm,
        scratch_shapes=[state, dma((1,))],
        compiler_params=pltpu.CompilerParams(vmem_limit_bytes=8 * 2**20),
    )(*parts)


def solution(mesh):
    placed = (
        P(None, ("patch", "sub"), None, None),
        P(("patch", "sub"), None, None),
        P(None, ("patch", "sub"), None, None),
        P(None, ("patch", "sub"), None, None),
        P(None, ("patch", "sub"), None, None),
        P(),
        P(("patch", "sub")),
        P(("patch", "sub"), None),
    )
    total = mesh.shape["patch"] * mesh.shape["sub"]
    return jax.shard_map(
        functools.partial(shards, total, mesh.shape["sub"]),
        mesh=mesh,
        in_specs=placed,
        out_specs=P(None, ("patch", "sub"), None, None),
        check_vma=False,
    )
```

```python
import functools

import jax
import jax.numpy as jnp
import numpy as np
from jax import lax
from jax.experimental import pallas as pl
from jax.experimental.pallas import tpu as pltpu
from jax.sharding import PartitionSpec as P

LOGICAL = pl.DeviceIdType.LOGICAL
ROWS = 8
cfl_number = 0.5
penalty_weight = 0.5


def circulant(points, extra):
    length = points + extra
    half = (length - 1) // 2
    waves = np.arange(1, half + 1, dtype=np.float64)
    weights = waves * (2.0 * np.pi * (points - 1) / length)
    shifts = np.arange(length)
    phase = 2.0 * np.pi / length * (waves[:, None] * shifts[None, :] % length)
    kernel = -(2.0 / length) * np.sum(weights[:, None] * np.sin(phase), axis=0)
    at = (np.arange(points)[:, None] - np.arange(length)[None, :]) % length
    full = kernel[at].astype(np.float32)
    padded = -(-extra // ROWS) * ROWS
    outer = np.zeros((padded, points), np.float32)
    outer[:extra] = full[:, points:].T
    return np.concatenate([full[:, :points].T, outer])


def split(x):
    hi = x.astype(jnp.bfloat16)
    lo = (x - hi.astype(jnp.float32)).astype(jnp.bfloat16)
    return hi, lo


def kernel(
    total, subs, offsets, reach,
    conn_hbm, count_hbm, fields_hbm, density_hbm, moduli_hbm, diag_hbm, cross_hbm,
    ext_hbm, consts_hbm,
    fld, rate1, rate2, cols, edges2, factors,
    conn, count, ext, consts,
    med, dxi, deta, left, right, ext_v, trans, thin, wide, tall, along, rims,
    lines, lines2, turned1, turned2, outbox1, outbox2, inbox1, inbox2,
    mine, gather, tally,
    load_sem, send_sem, recv_sem,
):
    comps, slots, n, _ = fld.shape
    sides = slots * 4
    chunks = n // ROWS
    me = lax.axis_index("patch") * subs + lax.axis_index("sub")
    simple = total & (total - 1) == 0
    unroll = total - 1 if total <= 64 else 1

    def away(off):
        return lax.rem(me + off, total)

    def peer(d):
        return me ^ d if simple else away(d)

    conn_load = pltpu.make_async_copy(conn_hbm, conn, load_sem.at[0])
    count_load = pltpu.make_async_copy(count_hbm, count, load_sem.at[1])
    ext_load = pltpu.make_async_copy(ext_hbm, ext, load_sem.at[2])
    consts_load = pltpu.make_async_copy(consts_hbm, consts, load_sem.at[3])
    fields_load = pltpu.make_async_copy(fields_hbm, fld, load_sem.at[4])
    med_load = pltpu.make_async_copy(med, med, load_sem.at[5])
    conn_load.start()
    ext_load.start()
    share = consts.shape[0] // 5
    for k in range(5):
        part = pl.ds(k * share, share)
        pltpu.make_async_copy(consts_hbm.at[part], consts.at[part], load_sem.at[3]).start()

    def fetch(src, dst, sem, cuts):
        for p in range(slots):
            for k in range(cuts):
                part = (p, pl.ds(k * (n // cuts), n // cuts))
                pltpu.make_async_copy(src.at[part], dst.at[part], sem).start()

    for f in range(comps):
        fetch(fields_hbm.at[f], fld.at[f], load_sem.at[4], 4)
    barrier = pltpu.get_barrier_semaphore()

    def greet(i, _):
        pl.semaphore_signal(
            barrier, inc=1, device_id=peer(1 + i), device_id_type=LOGICAL
        )
        return _

    lax.fori_loop(0, total - 1, greet, 0, unroll=unroll)
    count_load.start()
    fetch(density_hbm, med.at[0], load_sem.at[5], 2)
    for k in range(2):
        fetch(moduli_hbm.at[k], med.at[1 + k], load_sem.at[5], 2)
    for k in range(2):
        fetch(diag_hbm.at[k], med.at[3 + k], load_sem.at[5], 2)
        fetch(cross_hbm.at[k], med.at[5 + k], load_sem.at[5], 2)

    lines[...] = jnp.zeros_like(lines)
    lines2[...] = jnp.zeros_like(lines2)
    trans[...] = jnp.zeros_like(trans)
    ext_v[...] = jnp.zeros_like(ext_v)

    conn_load.wait()
    near = [away(off) for off in offsets]
    owner = [conn[0, s] for s in range(sides)]
    linked = [owner[s] >= 0 for s in range(sides)]
    strip = [jnp.where(linked[s], conn[1, s], 0) for s in range(sides)]
    flip = [conn[2, s] for s in range(sides)]
    tags = []
    for s in range(sides):
        rank = jnp.int32(0)
        for t in range(s):
            rank = rank + (owner[t] == owner[s]).astype(jnp.int32)
        tags.append(owner[s] * sides + rank)
    picks = []
    for there in near:
        pick = []
        for k in range(slots):
            tag, at = there * sides + k, jnp.int32(0)
            for s in range(1, sides):
                at = jnp.where(tags[s] == tag, s, at)
            pick.append(at)
        picks.append(pick)

    lane = lax.broadcasted_iota(jnp.int32, (ROWS, n), 1)
    row = lax.broadcasted_iota(jnp.int32, (ROWS, n), 0)
    low, high = lane == 0, lane == n - 1
    edge = low | high
    used = row < comps
    weight = penalty_weight * (n - 1)

    def collect(state, lines):
        kinds = state.shape[0]
        pairs = [(f, p, p * 8 + f) for p in range(slots) for f in range(kinds)]

        def columns(c, _):
            rows = pl.ds(pl.multiple_of(c * ROWS, ROWS), ROWS)
            acc = jnp.zeros((ROWS, n), jnp.float32)
            for f, p, m in pairs:
                turned = pltpu.roll(state[f, p, rows, :], 2 * m + 1, 1)
                acc = jnp.where((lane == 2 * m) | (lane == 2 * m + 1), turned, acc)
            cols[rows, :] = acc
            return _

        lax.fori_loop(0, chunks, columns, 0, unroll=chunks)
        trans[...] = jnp.transpose(cols[...])
        for p in range(slots):
            lines[p * 4 + 2] = trans[pl.ds(p * 16 + 1, 8, stride=2), :]
            lines[p * 4 + 3] = trans[pl.ds(p * 16, 8, stride=2), :]
            for f in range(kinds):
                lines[p * 4, pl.ds(f, 1)] = state[f, p, pl.ds(0, 1), :]
                lines[p * 4 + 1, pl.ds(f, 1)] = state[f, p, pl.ds(n - 1, 1), :]

    def turn(lines, turned):
        for s in range(sides):
            index = jnp.where(flip[s] == 1, n - 1 - lane, lane)
            turned[s] = jnp.take_along_axis(lines[s], index, axis=1)

    def post(turned, outbox, inbox, at, rider=None):
        for o in range(len(offsets)):
            for k in range(slots):
                line = turned[picks[o][k]]
                if rider is not None:
                    line = jnp.where(row == comps, rider, line)
                outbox[o * slots + k] = line
        height = comps + (rider is not None)
        for o in range(len(offsets)):
            spot = (pl.ds(o * slots, slots), pl.ds(0, height), slice(None))
            pltpu.make_async_remote_copy(
                src_ref=outbox.at[spot],
                dst_ref=inbox.at[spot],
                send_sem=send_sem.at[0],
                recv_sem=recv_sem.at[at],
                device_id=near[o],
                device_id_type=LOGICAL,
            ).start()

    def settle(buffer, sem):
        pltpu.make_async_copy(buffer, buffer, sem).wait()

    def carried(buffer, height):
        return buffer.at[:, pl.ds(0, height), :]

    def whole(value):
        return jnp.broadcast_to(value, (ROWS, n))

    def partners(turned, inbox):
        return [
            jnp.where(used, jnp.where(local[s], turned[strip[s]], inbox[box[s]]), 0.0)
            for s in range(sides)
        ]

    def spread(jump):
        for p in range(slots):
            trans[pl.ds(p * 16 + 1, 8, stride=2), :] = jump[p * 4 + 2]
            trans[pl.ds(p * 16, 8, stride=2), :] = jump[p * 4 + 3]
        cols[...] = jnp.transpose(trans[...])

    def derive(state):
        for f in range(comps):
            h0, l0 = split(state[f, 0])
            h1, l1 = split(state[f, 1])
            rows = jnp.concatenate(
                [jnp.concatenate([h0, l0], axis=1), jnp.concatenate([h1, l1], axis=1)], axis=0
            )
            eta = jnp.dot(rows, right[...], preferred_element_type=jnp.float32)
            both = eta[:, :n] + eta[:, n:]
            deta[f, 0] = both[:n]
            deta[f, 1] = both[n:]
            body = jnp.concatenate(
                [jnp.concatenate([h0, h1], axis=1), jnp.concatenate([l0, l1], axis=1)], axis=0
            )
            xi = jnp.dot(left[...], body, preferred_element_type=jnp.float32)
            both = xi[:n] + xi[n:]
            dxi[f, 0] = both[:, :n]
            dxi[f, 1] = both[:, n:]

    def interior(keep):
        for p in range(slots):

            def body(c, _):
                rows = pl.ds(pl.multiple_of(c * ROWS, ROWS), ROWS)
                inv, lame, shear, xx, yy, xy, ex = (med[k, p, rows, :] for k in range(7))
                stiff = lame + 2.0 * shear
                ax = [dxi[f, p, rows, :] for f in range(comps)]
                ay = [deta[f, p, rows, :] for f in range(comps)]
                gx = [xx * a + ex * b for a, b in zip(ax, ay)]
                gy = [xy * a + yy * b for a, b in zip(ax, ay)]
                keep(0, p, rows, (gx[2] + gy[4]) * inv)
                keep(1, p, rows, (gx[4] + gy[3]) * inv)
                keep(2, p, rows, stiff * gx[0] + lame * gy[1])
                keep(3, p, rows, lame * gx[0] + stiff * gy[1])
                keep(4, p, rows, shear * (gy[0] + gx[1]))
                return _

            lax.fori_loop(0, chunks, body, 0, unroll=chunks)

    fields_load.wait()
    ext_load.wait()
    consts_load.wait()
    twice, extra = ext.shape
    edges = twice // 2
    ext_v[pl.ds(0, twice), pl.ds(0, extra)] = ext[...]
    bent = jnp.dot(
        ext_v[...],
        consts[pl.ds(n, ext_v.shape[1]), :],
        precision=lax.Precision.HIGHEST,
        preferred_element_type=jnp.float32,
    )
    consts[pl.ds(n - edges, edges), :] = consts[pl.ds(n - edges, edges), :] + bent[:edges]
    consts[pl.ds(0, edges), :] = consts[pl.ds(0, edges), :] + bent[edges:twice]
    matrix = consts[pl.ds(0, n), :]
    hi, lo = split(matrix)
    none = jnp.zeros_like(hi)
    right[...] = jnp.concatenate(
        [jnp.concatenate([hi, lo], axis=1), jnp.concatenate([hi, none], axis=1)], axis=0
    )
    hi, lo = split(jnp.transpose(matrix))
    left[...] = jnp.concatenate(
        [jnp.concatenate([hi, hi], axis=1), jnp.concatenate([lo, none], axis=1)], axis=0
    )
    collect(fld, lines)
    turn(lines, turned1)
    table = jnp.zeros((ROWS, n), jnp.int32)
    for r in range(3):
        for s in range(sides):
            table = jnp.where(lane == r * sides + s, conn[r, s], table)
    table = table.astype(jnp.float32)

    pl.semaphore_wait(barrier, total - 1)
    post(turned1, outbox1, inbox1, 0, table)

    count_load.wait()
    med_load.wait()
    tile = jnp.zeros((ROWS, n), jnp.float32)
    place = lane - row * sides
    for p in range(slots):
        for b in range(2):
            first = p * 4 + 2 * b
            laid = pltpu.roll(lines[p * 4 + b], first + 1, 1, stride=sides, stride_axis=0)
            tile = jnp.where(used & ((place == first) | (place == first + 1)), laid, tile)
    packed = jnp.sum(tile, axis=0, keepdims=True)

    top = jnp.zeros((ROWS, n), jnp.float32)
    for p in range(slots):

        def speeds(c, top):
            rows = pl.ds(pl.multiple_of(c * ROWS, ROWS), ROWS)
            dens, lame, shear, xx, yy, xy, ex = (med[k, p, rows, :] for k in range(7))
            inv = 1.0 / dens
            med[0, p, rows, :] = inv
            along_x, along_y = xx * xx + xy * xy, ex * ex + yy * yy
            both = along_x * along_y
            square = along_x + along_y + 2.0 * (both * lax.rsqrt(both))
            return jnp.maximum(top, (lame + 2.0 * shear) * inv * square)

        part = lax.fori_loop(
            0, chunks, speeds, jnp.zeros((ROWS, n), jnp.float32), unroll=chunks
        )
        top = jnp.maximum(top, jnp.where(count[0] > p, part, 0.0))
    mine[...] = jnp.concatenate([jnp.max(top, axis=0, keepdims=True), packed], axis=0)

    def tell(i, _):
        d = total - 1 - i
        pltpu.make_async_remote_copy(
            src_ref=mine,
            dst_ref=gather.at[d - 1],
            send_sem=send_sem.at[0],
            recv_sem=recv_sem.at[1],
            device_id=peer(d),
            device_id_type=LOGICAL,
        ).start()
        return _

    lax.fori_loop(0, total - 1, tell, 0, unroll=unroll)

    derive(fld)

    def keep1(f, p, rows, value):
        rate1[f, p, rows, :] = value

    interior(keep1)
    collect(rate1, lines2)
    turn(lines2, turned2)
    post(turned2, outbox2, inbox2, 2)

    box, local = [], []
    for s in range(sides):
        pos = jnp.int32(0)
        for t in range(sides):
            if t != s:
                pos = pos + ((owner[t] == owner[s]) & (strip[t] < strip[s])).astype(jnp.int32)
        pos = jnp.minimum(pos, slots - 1)
        at = pos
        for o, off in enumerate(offsets):
            at = jnp.where(owner[s] == away(total - off), o * slots + pos, at)
        box.append(at)
        local.append(owner[s] == me)

    def keep2(f, p, rows, value):
        rate2[f, p, rows, :] = value

    derive(rate1)
    interior(keep2)
    collect(med, rims)
    block = lax.broadcasted_iota(jnp.int32, (n, n), 1)
    matrix = jnp.transpose(consts[pl.ds(0, n), :])
    hi = matrix.astype(jnp.bfloat16).astype(jnp.float32)
    thin[...] = jnp.where(
        block < 2,
        pltpu.roll(hi, 1, 1),
        jnp.where(
            block < 4,
            pltpu.roll(hi, 3, 1),
            jnp.where(block < 6, pltpu.roll(matrix - hi, 5, 1), 0.0),
        ),
    ).astype(jnp.bfloat16)
    tall[...] = jnp.zeros_like(tall)
    wide[...] = jnp.zeros_like(wide)
    first, last = consts[pl.ds(0, 1), :], consts[pl.ds(n - 1, 1), :]
    deep = lax.broadcasted_iota(jnp.int32, (2 * ROWS, n), 0)

    def pieces(value):
        hi = value.astype(jnp.bfloat16).astype(jnp.float32)
        return hi, value - hi

    first_hi, first_lo = pieces(first)
    last_hi, last_lo = pieces(last)
    for k, (one, two) in enumerate(
        ((first_hi, last_hi), (first_hi, last_hi), (first_lo, last_lo))
    ):
        one = jnp.broadcast_to(one, (2 * ROWS, n))
        two = jnp.broadcast_to(two, (2 * ROWS, n))
        for f in range(comps):
            slab = jnp.where(deep == 2 * f + 1, one, jnp.where(deep == 2 * f, two, 0.0))
            slab = slab.astype(jnp.bfloat16)
            for p in range(slots):
                wide[pl.ds((k * slots + p) * 16, 16), pl.ds((f * slots + p) * n, n)] = slab

    settle(carried(inbox1, comps + 1), recv_sem.at[0])
    other = partners(turned1, inbox1)
    jump1 = [jnp.where(linked[s], weight * (other[s] - lines[s]), 0.0) for s in range(sides)]
    for p in range(slots):
        parts = [pieces(jump1[p * 4 + side]) for side in range(4)]
        for k, at in enumerate((0, 1, 0)):
            low_rows = (k * slots + p) * 16
            trans[pl.ds(low_rows + 1, 8, stride=2), :] = parts[2][at]
            trans[pl.ds(low_rows, 8, stride=2), :] = parts[3][at]
        (west_hi, west_lo), (east_hi, east_lo) = parts[0], parts[1]
        for f in range(comps):
            near_hi, near_lo = whole(west_hi[f : f + 1]), whole(west_lo[f : f + 1])
            far_hi, far_lo = whole(east_hi[f : f + 1]), whole(east_lo[f : f + 1])
            slab = jnp.where((row == 1) | (row == 5), near_hi, 0.0)
            slab = jnp.where((row == 0) | (row == 4), far_hi, slab)
            slab = jnp.where(row == 2, far_lo, jnp.where(row == 3, near_lo, slab))
            slab = jnp.concatenate([slab, jnp.zeros_like(slab)], axis=0)
            tall[pl.ds(0, 16), pl.ds((f * slots + p) * n, n)] = slab.astype(jnp.bfloat16)
    stacked = jnp.concatenate(jump1, axis=0)
    hi, lo = split(stacked)
    slope = jnp.dot(
        jnp.concatenate([hi, lo], axis=1), right[...], preferred_element_type=jnp.float32
    )
    slope = slope[:, :n] + slope[:, n:]
    for s in range(sides):
        along[s] = slope[s * ROWS : (s + 1) * ROWS]
    for f in range(comps):
        span = pl.ds(f * slots * n, slots * n)
        xi = jnp.dot(thin[...], tall[:, span], preferred_element_type=jnp.float32)
        for p in range(slots):
            dxi[f, p] = xi[:, p * n : (p + 1) * n]
    upright = jnp.transpose(trans[...]).astype(jnp.bfloat16)
    for f in range(comps):
        span = pl.ds(f * slots * n, slots * n)
        eta = jnp.dot(upright, wide[:, span], preferred_element_type=jnp.float32)
        for p in range(slots):
            deta[f, p] = eta[:, p * n : (p + 1) * n]

    def keep3(f, p, rows, value):
        rate2[f, p, rows, :] = rate2[f, p, rows, :] + value

    interior(keep3)
    for s in range(sides):
        inv, lame, shear, xx, yy, xy, ex = (rims[s, pl.ds(k, 1), :] for k in range(7))
        stiff = lame + 2.0 * shear
        lean = [along[s, pl.ds(f, 1), :] for f in range(comps)]
        to_x, to_y = (ex, yy) if s % 4 < 2 else (xx, xy)
        gx = [to_x * a for a in lean]
        gy = [to_y * a for a in lean]
        along[s, pl.ds(0, 1), :] = (gx[2] + gy[4]) * inv
        along[s, pl.ds(1, 1), :] = (gx[4] + gy[3]) * inv
        along[s, pl.ds(2, 1), :] = stiff * gx[0] + lame * gy[1]
        along[s, pl.ds(3, 1), :] = lame * gx[0] + stiff * gy[1]
        along[s, pl.ds(4, 1), :] = shear * (gy[0] + gx[1])

    their_owner = jnp.full((ROWS, n), -1, jnp.int32)
    their_strip = jnp.zeros((ROWS, n), jnp.int32)
    their_flip = jnp.zeros((ROWS, n), jnp.int32)
    for s in range(sides):
        here = lax.shift_right_logical(lane, 1) == s
        their_owner = jnp.where(here, owner[s], their_owner)
        their_strip = jnp.where(here, strip[s], their_strip)
        their_flip = jnp.where(here, flip[s], their_flip)

    def seat(device, count):
        at = jnp.zeros((ROWS, n), jnp.int32)
        for j in range(1, count):
            at = jnp.where(device == away(reach[j]), j, at)
        return at

    def nook(strip, end):
        b = strip & 1
        across = (strip & 2) == 0
        return (strip & ~3) + jnp.where(across, 2 * b + 1 - end, 2 * end + 1 - b)

    def look(rows, seats, index):
        found = jnp.zeros((ROWS, n), jnp.float32)
        index = row * sides + index
        for j, line in enumerate(rows):
            found = jnp.where(seats == j, jnp.take_along_axis(line, index, axis=1), found)
        return found

    close = 1 + len(offsets)
    tables = [table]
    for j in range(1, close):
        o = offsets.index(total - reach[j])
        tables.append(whole(inbox1[o * slots, pl.ds(comps, 1), :]))
    end = (1 - (lane & 1)) ^ (their_flip & 1)
    base = seat(their_owner, close)
    beside = (their_strip & ~3) + jnp.where((their_strip & 2) == 0, 2 + end, end)
    entry = look(tables, base, beside)
    far_owner, far_strip, far_flip = (whole(entry[r : r + 1]).astype(jnp.int32) for r in range(3))
    far_strip = jnp.where(far_owner >= 0, far_strip, 0)
    far_end = (their_strip & 1) ^ (far_flip & 1)
    far_seat = seat(far_owner, len(reach))
    far_nook = nook(far_strip, far_end)
    near_nook = nook(their_strip, end)

    rest = []
    for p in range(slots):
        west, east, south, north = jump1[p * 4 : p * 4 + 4]
        mixed = (
            jnp.where(low, south, 0.0) + jnp.where(high, pltpu.roll(north, n - 1, 1), 0.0),
            jnp.where(low, pltpu.roll(south, 1, 1), 0.0) + jnp.where(high, north, 0.0),
            jnp.where(low, west, 0.0) + jnp.where(high, pltpu.roll(east, n - 1, 1), 0.0),
            jnp.where(low, pltpu.roll(west, 1, 1), 0.0) + jnp.where(high, east, 0.0),
        )
        for side in range(4):
            s = p * 4 + side
            rest.append(-mixed[side] - 2.0 * jump1[s] - lines2[s])

    settle(gather, recv_sem.at[1])

    def report(off):
        if simple:
            return gather[(me ^ away(off)) - 1, 1:]
        return gather[total - off - 1, 1:]

    reports = [whole(mine[1:])] + [whole(report(off)) for off in reach[1:]]
    value = look(reports, far_seat, far_nook)
    own = look(reports[:close], base, near_nook)
    bend = jnp.where((far_owner >= 0) & used, weight * (value - own), 0.0)
    best = [mine[:1]] + [gather[d, :1] for d in range(total - 1)]
    while len(best) > 1:
        best = [jnp.maximum(*best[k : k + 2]) if k + 1 < len(best) else best[k]
                for k in range(0, len(best), 2)]
    bound = jnp.sqrt(jnp.max(best[0], axis=1, keepdims=True))
    step = jnp.broadcast_to(cfl_number / (bound * (n - 1)), (ROWS, n))
    half = 0.5 * step * step
    factors[0] = step
    factors[1] = half
    for p in range(slots):
        factors[2 + p] = jnp.where(count[0] > p, 1.0, 0.0) + jnp.zeros((ROWS, n), jnp.float32)
    early = [step * jump1[s] + half * along[s] for s in range(sides)]
    for s in range(sides):
        rest[s] = rest[s] + jnp.where(edge, pltpu.roll(bend, n - (2 * s + 1), 1), 0.0)

    settle(carried(inbox2, comps), recv_sem.at[2])
    other = partners(turned2, inbox2)
    jump2 = [
        early[s] + jnp.where(linked[s], (half * weight) * (other[s] + rest[s]), 0.0)
        for s in range(sides)
    ]
    spread(jump2)
    for s in range(sides):
        edges2[s] = jump2[s]

    settle(tally, send_sem.at[0])


def finish(fld, rate1, rate2, cols, edges2, factors, out_hbm, out_v, sem):
    comps, slots, n, _ = fld.shape
    chunks = n // ROWS
    lane = lax.broadcasted_iota(jnp.int32, (ROWS, n), 1)
    row = lax.broadcasted_iota(jnp.int32, (ROWS, n), 0)
    edge = (lane == 0) | (lane == n - 1)
    step, half = factors[0], factors[1]
    for p in range(slots):
        live = factors[2 + p] > 0.0
        for f in range(comps):
            for c in range(chunks):
                rows = pl.ds(c * ROWS, ROWS)
                side = pltpu.roll(cols[rows, :], n - (2 * (p * 8 + f) + 1), 1)
                value = fld[f, p, rows, :] + step * rate1[f, p, rows, :]
                value = value + half * rate2[f, p, rows, :] + jnp.where(edge, side, 0.0)
                for side, at in ((0, 0), (1, chunks - 1)):
                    if c == at:
                        line = jnp.broadcast_to(edges2[p * 4 + side, pl.ds(f, 1), :], (ROWS, n))
                        value = value + jnp.where(row == side * (ROWS - 1), line, 0.0)
                out_v[f, p, rows, :] = jnp.where(live, value, 0.0)
                if (c + 1) % 4 == 0:
                    part = (f, p, pl.ds((c - 3) * ROWS, 4 * ROWS))
                    pltpu.make_async_copy(out_v.at[part], out_hbm.at[part], sem.at[0]).start()
    pltpu.make_async_copy(out_v, out_hbm, sem.at[0]).wait()


def shards(
    total, subs, fields, density, moduli, metric_diag, metric_cross, extension, count, connectivity
):
    comps, slots, n, _ = fields.shape
    consts = circulant(n, extension.shape[0])
    far = total // 2 + 1
    offsets = (1, total - 1, far, total - far)
    reach = [0, *offsets]
    for a in offsets:
        for b in offsets:
            if (a + b) % total not in reach:
                reach.append((a + b) % total)
    f32, i32 = jnp.float32, jnp.int32
    hbm = pl.BlockSpec(memory_space=pltpu.HBM)
    state = pltpu.VMEM(fields.shape, f32)
    square = pltpu.VMEM((n, n), f32)
    dma = pltpu.SemaphoreType.DMA
    boxed = pltpu.VMEM((len(offsets) * slots, 8, n), f32)
    strips = pltpu.VMEM((slots * 4, 8, n), f32)
    factors = pltpu.VMEM((2 + slots, ROWS, n), f32)
    vmem = pl.BlockSpec(memory_space=pltpu.VMEM)
    parts = pl.pallas_call(
        functools.partial(kernel, total, subs, offsets, reach),
        out_shape=[state, state, state, square, strips, factors],
        in_specs=[hbm] * 9,
        out_specs=[vmem] * 6,
        scratch_shapes=[
            pltpu.SMEM(connectivity.shape[::-1], i32),
            pltpu.SMEM(count.shape, i32),
            pltpu.VMEM(extension.shape[::-1], f32),
            pltpu.VMEM(consts.shape, f32),
            pltpu.VMEM((7,) + density.shape, f32),
            state, state,
            pltpu.VMEM((2 * n, 2 * n), jnp.bfloat16),
            pltpu.VMEM((2 * n, 2 * n), jnp.bfloat16),
            pltpu.VMEM((-(-extension.shape[1] // ROWS) * ROWS, consts.shape[0] - n), f32),
            square,
            pltpu.VMEM((n, n), jnp.bfloat16),
            pltpu.VMEM((n, comps * slots * n), jnp.bfloat16),
            pltpu.VMEM((n, comps * slots * n), jnp.bfloat16),
            strips, strips,
            strips, strips, strips, strips,
            boxed, boxed, boxed, boxed,
            pltpu.VMEM((2, n), f32),
            pltpu.VMEM((total - 1, 2, n), f32),
            pltpu.VMEM((total - 1 + len(offsets) * slots * (2 * comps + 1) // 2, 2, n), f32),
            dma((6,)), dma((1,)), dma((3,)),
        ],
        compiler_params=pltpu.CompilerParams(collective_id=0, has_side_effects=True),
    )(connectivity.T, count, fields, density, moduli, metric_diag, metric_cross, extension.T,
      jnp.asarray(consts))
    return pl.pallas_call(
        finish,
        out_shape=jax.ShapeDtypeStruct(fields.shape, f32),
        in_specs=[vmem] * 6,
        out_specs=hbm,
        scratch_shapes=[state, dma((1,))],
        compiler_params=pltpu.CompilerParams(vmem_limit_bytes=8 * 2**20),
    )(*parts)


def solution(mesh):
    placed = (
        P(None, ("patch", "sub"), None, None),
        P(("patch", "sub"), None, None),
        P(None, ("patch", "sub"), None, None),
        P(None, ("patch", "sub"), None, None),
        P(None, ("patch", "sub"), None, None),
        P(),
        P(("patch", "sub")),
        P(("patch", "sub"), None),
    )
    total = mesh.shape["patch"] * mesh.shape["sub"]
    return jax.shard_map(
        functools.partial(shards, total, mesh.shape["sub"]),
        mesh=mesh,
        in_specs=placed,
        out_specs=P(None, ("patch", "sub"), None, None),
        check_vma=False,
    )
```

```python
import functools

import jax
import jax.numpy as jnp
import numpy as np
from jax import lax
from jax.experimental import pallas as pl
from jax.experimental.pallas import tpu as pltpu
from jax.sharding import PartitionSpec as P

LOGICAL = pl.DeviceIdType.LOGICAL
ROWS = 8
cfl_number = 0.5
penalty_weight = 0.5


def circulant(points, extra):
    length = points + extra
    half = (length - 1) // 2
    waves = np.arange(1, half + 1, dtype=np.float64)
    weights = waves * (2.0 * np.pi * (points - 1) / length)
    shifts = np.arange(length)
    phase = 2.0 * np.pi / length * (waves[:, None] * shifts[None, :] % length)
    kernel = -(2.0 / length) * np.sum(weights[:, None] * np.sin(phase), axis=0)
    at = (np.arange(points)[:, None] - np.arange(length)[None, :]) % length
    full = kernel[at].astype(np.float32)
    padded = -(-extra // ROWS) * ROWS
    outer = np.zeros((padded, points), np.float32)
    outer[:extra] = full[:, points:].T
    return np.concatenate([full[:, :points].T, outer])


def split(x):
    hi = x.astype(jnp.bfloat16)
    lo = (x - hi.astype(jnp.float32)).astype(jnp.bfloat16)
    return hi, lo


def kernel(
    total, subs, offsets, reach,
    conn_hbm, count_hbm, fields_hbm, density_hbm, moduli_hbm, diag_hbm, cross_hbm,
    ext_hbm, consts_hbm,
    fld, rate1, rate2, cols, edges2, factors,
    conn, count, ext, consts,
    med, dxi, deta, left, right, ext_v, trans, thin, wide, tall, along, rims,
    lines, lines2, turned1, turned2, outbox1, outbox2, inbox1, inbox2,
    mine, gather, tally,
    load_sem, send_sem, recv_sem,
):
    comps, slots, n, _ = fld.shape
    sides = slots * 4
    chunks = n // ROWS
    me = lax.axis_index("patch") * subs + lax.axis_index("sub")
    simple = total & (total - 1) == 0
    unroll = total - 1 if total <= 64 else 1

    def away(off):
        return lax.rem(me + off, total)

    def peer(d):
        return me ^ d if simple else away(d)

    conn_load = pltpu.make_async_copy(conn_hbm, conn, load_sem.at[0])
    count_load = pltpu.make_async_copy(count_hbm, count, load_sem.at[1])
    ext_load = pltpu.make_async_copy(ext_hbm, ext, load_sem.at[2])
    consts_load = pltpu.make_async_copy(consts_hbm, consts, load_sem.at[3])
    fields_load = pltpu.make_async_copy(fields_hbm, fld, load_sem.at[4])
    med_load = pltpu.make_async_copy(med, med, load_sem.at[5])
    conn_load.start()
    ext_load.start()
    share = consts.shape[0] // 5
    for k in range(5):
        part = pl.ds(k * share, share)
        pltpu.make_async_copy(consts_hbm.at[part], consts.at[part], load_sem.at[3]).start()

    def fetch(src, dst, sem, cuts):
        for p in range(slots):
            for k in range(cuts):
                part = (p, pl.ds(k * (n // cuts), n // cuts))
                pltpu.make_async_copy(src.at[part], dst.at[part], sem).start()

    for f in range(comps):
        fetch(fields_hbm.at[f], fld.at[f], load_sem.at[4], 4)
    barrier = pltpu.get_barrier_semaphore()

    def greet(i, _):
        pl.semaphore_signal(
            barrier, inc=1, device_id=peer(1 + i), device_id_type=LOGICAL
        )
        return _

    lax.fori_loop(0, total - 1, greet, 0, unroll=unroll)
    count_load.start()
    fetch(density_hbm, med.at[0], load_sem.at[5], 2)
    for k in range(2):
        fetch(moduli_hbm.at[k], med.at[1 + k], load_sem.at[5], 2)
    for k in range(2):
        fetch(diag_hbm.at[k], med.at[3 + k], load_sem.at[5], 2)
        fetch(cross_hbm.at[k], med.at[5 + k], load_sem.at[5], 2)

    lines[...] = jnp.zeros_like(lines)
    lines2[...] = jnp.zeros_like(lines2)
    trans[...] = jnp.zeros_like(trans)
    ext_v[...] = jnp.zeros_like(ext_v)

    conn_load.wait()
    near = [away(off) for off in offsets]
    owner = [conn[0, s] for s in range(sides)]
    linked = [owner[s] >= 0 for s in range(sides)]
    strip = [jnp.where(linked[s], conn[1, s], 0) for s in range(sides)]
    flip = [conn[2, s] for s in range(sides)]
    tags = []
    for s in range(sides):
        rank = jnp.int32(0)
        for t in range(s):
            rank = rank + (owner[t] == owner[s]).astype(jnp.int32)
        tags.append(owner[s] * sides + rank)
    picks = []
    for there in near:
        pick = []
        for k in range(slots):
            tag, at = there * sides + k, jnp.int32(0)
            for s in range(1, sides):
                at = jnp.where(tags[s] == tag, s, at)
            pick.append(at)
        picks.append(pick)

    lane = lax.broadcasted_iota(jnp.int32, (ROWS, n), 1)
    row = lax.broadcasted_iota(jnp.int32, (ROWS, n), 0)
    low, high = lane == 0, lane == n - 1
    edge = low | high
    used = row < comps
    weight = penalty_weight * (n - 1)

    def collect(state, lines):
        kinds = state.shape[0]
        pairs = [(f, p, p * 8 + f) for p in range(slots) for f in range(kinds)]

        def columns(c, _):
            rows = pl.ds(pl.multiple_of(c * ROWS, ROWS), ROWS)
            acc = jnp.zeros((ROWS, n), jnp.float32)
            for f, p, m in pairs:
                turned = pltpu.roll(state[f, p, rows, :], 2 * m + 1, 1)
                acc = jnp.where((lane == 2 * m) | (lane == 2 * m + 1), turned, acc)
            cols[rows, :] = acc
            return _

        lax.fori_loop(0, chunks, columns, 0, unroll=chunks)
        trans[...] = jnp.transpose(cols[...])
        for p in range(slots):
            lines[p * 4 + 2] = trans[pl.ds(p * 16 + 1, 8, stride=2), :]
            lines[p * 4 + 3] = trans[pl.ds(p * 16, 8, stride=2), :]
            for f in range(kinds):
                lines[p * 4, pl.ds(f, 1)] = state[f, p, pl.ds(0, 1), :]
                lines[p * 4 + 1, pl.ds(f, 1)] = state[f, p, pl.ds(n - 1, 1), :]

    def turn(lines, turned):
        for s in range(sides):
            index = jnp.where(flip[s] == 1, n - 1 - lane, lane)
            turned[s] = jnp.take_along_axis(lines[s], index, axis=1)

    def post(turned, outbox, inbox, at, rider=None):
        for o in range(len(offsets)):
            for k in range(slots):
                line = turned[picks[o][k]]
                if rider is not None:
                    line = jnp.where(row == comps, rider, line)
                outbox[o * slots + k] = line
        height = comps + (rider is not None)
        for o in range(len(offsets)):
            spot = (pl.ds(o * slots, slots), pl.ds(0, height), slice(None))
            pltpu.make_async_remote_copy(
                src_ref=outbox.at[spot],
                dst_ref=inbox.at[spot],
                send_sem=send_sem.at[0],
                recv_sem=recv_sem.at[at],
                device_id=near[o],
                device_id_type=LOGICAL,
            ).start()

    def settle(buffer, sem):
        pltpu.make_async_copy(buffer, buffer, sem).wait()

    def carried(buffer, height):
        return buffer.at[:, pl.ds(0, height), :]

    def whole(value):
        return jnp.broadcast_to(value, (ROWS, n))

    def partners(turned, inbox):
        return [
            jnp.where(used, jnp.where(local[s], turned[strip[s]], inbox[box[s]]), 0.0)
            for s in range(sides)
        ]

    def spread(jump):
        for p in range(slots):
            trans[pl.ds(p * 16 + 1, 8, stride=2), :] = jump[p * 4 + 2]
            trans[pl.ds(p * 16, 8, stride=2), :] = jump[p * 4 + 3]
        cols[...] = jnp.transpose(trans[...])

    def derive(state):
        for f in range(comps):
            h0, l0 = split(state[f, 0])
            h1, l1 = split(state[f, 1])
            rows = jnp.concatenate(
                [jnp.concatenate([h0, l0], axis=1), jnp.concatenate([h1, l1], axis=1)], axis=0
            )
            eta = jnp.dot(rows, right[...], preferred_element_type=jnp.float32)
            both = eta[:, :n] + eta[:, n:]
            deta[f, 0] = both[:n]
            deta[f, 1] = both[n:]
            body = jnp.concatenate(
                [jnp.concatenate([h0, h1], axis=1), jnp.concatenate([l0, l1], axis=1)], axis=0
            )
            xi = jnp.dot(left[...], body, preferred_element_type=jnp.float32)
            both = xi[:n] + xi[n:]
            dxi[f, 0] = both[:, :n]
            dxi[f, 1] = both[:, n:]

    def interior(keep):
        for p in range(slots):

            def body(c, _):
                rows = pl.ds(pl.multiple_of(c * ROWS, ROWS), ROWS)
                inv, lame, shear, xx, yy, xy, ex = (med[k, p, rows, :] for k in range(7))
                stiff = lame + 2.0 * shear
                ax = [dxi[f, p, rows, :] for f in range(comps)]
                ay = [deta[f, p, rows, :] for f in range(comps)]
                gx = [xx * a + ex * b for a, b in zip(ax, ay)]
                gy = [xy * a + yy * b for a, b in zip(ax, ay)]
                keep(0, p, rows, (gx[2] + gy[4]) * inv)
                keep(1, p, rows, (gx[4] + gy[3]) * inv)
                keep(2, p, rows, stiff * gx[0] + lame * gy[1])
                keep(3, p, rows, lame * gx[0] + stiff * gy[1])
                keep(4, p, rows, shear * (gy[0] + gx[1]))
                return _

            lax.fori_loop(0, chunks, body, 0, unroll=chunks)

    fields_load.wait()
    ext_load.wait()
    consts_load.wait()
    twice, extra = ext.shape
    edges = twice // 2
    ext_v[pl.ds(0, twice), pl.ds(0, extra)] = ext[...]
    bent = jnp.dot(
        ext_v[...],
        consts[pl.ds(n, ext_v.shape[1]), :],
        precision=lax.Precision.HIGHEST,
        preferred_element_type=jnp.float32,
    )
    consts[pl.ds(n - edges, edges), :] = consts[pl.ds(n - edges, edges), :] + bent[:edges]
    consts[pl.ds(0, edges), :] = consts[pl.ds(0, edges), :] + bent[edges:twice]
    matrix = consts[pl.ds(0, n), :]
    hi, lo = split(matrix)
    none = jnp.zeros_like(hi)
    right[...] = jnp.concatenate(
        [jnp.concatenate([hi, lo], axis=1), jnp.concatenate([hi, none], axis=1)], axis=0
    )
    hi, lo = split(jnp.transpose(matrix))
    left[...] = jnp.concatenate(
        [jnp.concatenate([hi, hi], axis=1), jnp.concatenate([lo, none], axis=1)], axis=0
    )
    collect(fld, lines)
    turn(lines, turned1)
    table = jnp.zeros((ROWS, n), jnp.int32)
    for r in range(3):
        for s in range(sides):
            table = jnp.where(lane == r * sides + s, conn[r, s], table)
    table = table.astype(jnp.float32)

    pl.semaphore_wait(barrier, total - 1)
    post(turned1, outbox1, inbox1, 0, table)

    count_load.wait()
    med_load.wait()
    tile = jnp.zeros((ROWS, n), jnp.float32)
    place = lane - row * sides
    for p in range(slots):
        for b in range(2):
            first = p * 4 + 2 * b
            laid = pltpu.roll(lines[p * 4 + b], first + 1, 1, stride=sides, stride_axis=0)
            tile = jnp.where(used & ((place == first) | (place == first + 1)), laid, tile)
    packed = jnp.sum(tile, axis=0, keepdims=True)

    top = jnp.zeros((ROWS, n), jnp.float32)
    for p in range(slots):

        def speeds(c, top):
            rows = pl.ds(pl.multiple_of(c * ROWS, ROWS), ROWS)
            dens, lame, shear, xx, yy, xy, ex = (med[k, p, rows, :] for k in range(7))
            inv = 1.0 / dens
            med[0, p, rows, :] = inv
            along_x, along_y = xx * xx + xy * xy, ex * ex + yy * yy
            both = along_x * along_y
            square = along_x + along_y + 2.0 * (both * lax.rsqrt(both))
            return jnp.maximum(top, (lame + 2.0 * shear) * inv * square)

        part = lax.fori_loop(
            0, chunks, speeds, jnp.zeros((ROWS, n), jnp.float32), unroll=chunks
        )
        top = jnp.maximum(top, jnp.where(count[0] > p, part, 0.0))
    mine[...] = jnp.concatenate([jnp.max(top, axis=0, keepdims=True), packed], axis=0)

    def tell(i, _):
        d = total - 1 - i
        pltpu.make_async_remote_copy(
            src_ref=mine,
            dst_ref=gather.at[d - 1],
            send_sem=send_sem.at[0],
            recv_sem=recv_sem.at[1],
            device_id=peer(d),
            device_id_type=LOGICAL,
        ).start()
        return _

    lax.fori_loop(0, total - 1, tell, 0, unroll=unroll)

    derive(fld)

    def keep1(f, p, rows, value):
        rate1[f, p, rows, :] = value

    interior(keep1)
    collect(rate1, lines2)
    turn(lines2, turned2)
    post(turned2, outbox2, inbox2, 2)

    box, local = [], []
    for s in range(sides):
        pos = jnp.int32(0)
        for t in range(sides):
            if t != s:
                pos = pos + ((owner[t] == owner[s]) & (strip[t] < strip[s])).astype(jnp.int32)
        pos = jnp.minimum(pos, slots - 1)
        at = pos
        for o, off in enumerate(offsets):
            at = jnp.where(owner[s] == away(total - off), o * slots + pos, at)
        box.append(at)
        local.append(owner[s] == me)

    def keep2(f, p, rows, value):
        rate2[f, p, rows, :] = value

    derive(rate1)
    interior(keep2)
    collect(med, rims)
    block = lax.broadcasted_iota(jnp.int32, (n, n), 1)
    matrix = jnp.transpose(consts[pl.ds(0, n), :])
    hi = matrix.astype(jnp.bfloat16).astype(jnp.float32)
    thin[...] = jnp.where(
        block < 2,
        pltpu.roll(hi, 1, 1),
        jnp.where(
            block < 4,
            pltpu.roll(hi, 3, 1),
            jnp.where(block < 6, pltpu.roll(matrix - hi, 5, 1), 0.0),
        ),
    ).astype(jnp.bfloat16)
    tall[...] = jnp.zeros_like(tall)
    wide[...] = jnp.zeros_like(wide)
    first, last = consts[pl.ds(0, 1), :], consts[pl.ds(n - 1, 1), :]
    deep = lax.broadcasted_iota(jnp.int32, (2 * ROWS, n), 0)

    def pieces(value):
        hi = value.astype(jnp.bfloat16).astype(jnp.float32)
        return hi, value - hi

    first_hi, first_lo = pieces(first)
    last_hi, last_lo = pieces(last)
    for k, (one, two) in enumerate(
        ((first_hi, last_hi), (first_hi, last_hi), (first_lo, last_lo))
    ):
        one = jnp.broadcast_to(one, (2 * ROWS, n))
        two = jnp.broadcast_to(two, (2 * ROWS, n))
        for f in range(comps):
            slab = jnp.where(deep == 2 * f + 1, one, jnp.where(deep == 2 * f, two, 0.0))
            slab = slab.astype(jnp.bfloat16)
            for p in range(slots):
                wide[pl.ds((k * slots + p) * 16, 16), pl.ds((f * slots + p) * n, n)] = slab

    settle(carried(inbox1, comps + 1), recv_sem.at[0])
    other = partners(turned1, inbox1)
    jump1 = [jnp.where(linked[s], weight * (other[s] - lines[s]), 0.0) for s in range(sides)]
    for p in range(slots):
        parts = [pieces(jump1[p * 4 + side]) for side in range(4)]
        for k, at in enumerate((0, 1, 0)):
            low_rows = (k * slots + p) * 16
            trans[pl.ds(low_rows + 1, 8, stride=2), :] = parts[2][at]
            trans[pl.ds(low_rows, 8, stride=2), :] = parts[3][at]
        (west_hi, west_lo), (east_hi, east_lo) = parts[0], parts[1]
        for f in range(comps):
            near_hi, near_lo = whole(west_hi[f : f + 1]), whole(west_lo[f : f + 1])
            far_hi, far_lo = whole(east_hi[f : f + 1]), whole(east_lo[f : f + 1])
            slab = jnp.where((row == 1) | (row == 5), near_hi, 0.0)
            slab = jnp.where((row == 0) | (row == 4), far_hi, slab)
            slab = jnp.where(row == 2, far_lo, jnp.where(row == 3, near_lo, slab))
            slab = jnp.concatenate([slab, jnp.zeros_like(slab)], axis=0)
            tall[pl.ds(0, 16), pl.ds((f * slots + p) * n, n)] = slab.astype(jnp.bfloat16)
    stacked = jnp.concatenate(jump1, axis=0)
    hi, lo = split(stacked)
    slope = jnp.dot(
        jnp.concatenate([hi, lo], axis=1), right[...], preferred_element_type=jnp.float32
    )
    slope = slope[:, :n] + slope[:, n:]
    for s in range(sides):
        along[s] = slope[s * ROWS : (s + 1) * ROWS]
    for f in range(comps):
        span = pl.ds(f * slots * n, slots * n)
        xi = jnp.dot(thin[...], tall[:, span], preferred_element_type=jnp.float32)
        for p in range(slots):
            dxi[f, p] = xi[:, p * n : (p + 1) * n]
    upright = jnp.transpose(trans[...]).astype(jnp.bfloat16)
    for f in range(comps):
        span = pl.ds(f * slots * n, slots * n)
        eta = jnp.dot(upright, wide[:, span], preferred_element_type=jnp.float32)
        for p in range(slots):
            deta[f, p] = eta[:, p * n : (p + 1) * n]

    def keep3(f, p, rows, value):
        rate2[f, p, rows, :] = rate2[f, p, rows, :] + value

    interior(keep3)
    for s in range(sides):
        inv, lame, shear, xx, yy, xy, ex = (rims[s, pl.ds(k, 1), :] for k in range(7))
        stiff = lame + 2.0 * shear
        lean = [along[s, pl.ds(f, 1), :] for f in range(comps)]
        to_x, to_y = (ex, yy) if s % 4 < 2 else (xx, xy)
        gx = [to_x * a for a in lean]
        gy = [to_y * a for a in lean]
        along[s, pl.ds(0, 1), :] = (gx[2] + gy[4]) * inv
        along[s, pl.ds(1, 1), :] = (gx[4] + gy[3]) * inv
        along[s, pl.ds(2, 1), :] = stiff * gx[0] + lame * gy[1]
        along[s, pl.ds(3, 1), :] = lame * gx[0] + stiff * gy[1]
        along[s, pl.ds(4, 1), :] = shear * (gy[0] + gx[1])

    their_owner = jnp.full((ROWS, n), -1, jnp.int32)
    their_strip = jnp.zeros((ROWS, n), jnp.int32)
    their_flip = jnp.zeros((ROWS, n), jnp.int32)
    for s in range(sides):
        here = lax.shift_right_logical(lane, 1) == s
        their_owner = jnp.where(here, owner[s], their_owner)
        their_strip = jnp.where(here, strip[s], their_strip)
        their_flip = jnp.where(here, flip[s], their_flip)

    def seat(device, count):
        at = jnp.zeros((ROWS, n), jnp.int32)
        for j in range(1, count):
            at = jnp.where(device == away(reach[j]), j, at)
        return at

    def nook(strip, end):
        b = strip & 1
        across = (strip & 2) == 0
        return (strip & ~3) + jnp.where(across, 2 * b + 1 - end, 2 * end + 1 - b)

    def look(rows, seats, index):
        found = jnp.zeros((ROWS, n), jnp.float32)
        index = row * sides + index
        for j, line in enumerate(rows):
            found = jnp.where(seats == j, jnp.take_along_axis(line, index, axis=1), found)
        return found

    close = 1 + len(offsets)
    tables = [table]
    for j in range(1, close):
        o = offsets.index(total - reach[j])
        tables.append(whole(inbox1[o * slots, pl.ds(comps, 1), :]))
    end = (1 - (lane & 1)) ^ (their_flip & 1)
    base = seat(their_owner, close)
    beside = (their_strip & ~3) + jnp.where((their_strip & 2) == 0, 2 + end, end)
    entry = look(tables, base, beside)
    far_owner, far_strip, far_flip = (whole(entry[r : r + 1]).astype(jnp.int32) for r in range(3))
    far_strip = jnp.where(far_owner >= 0, far_strip, 0)
    far_end = (their_strip & 1) ^ (far_flip & 1)
    far_seat = seat(far_owner, len(reach))
    far_nook = nook(far_strip, far_end)
    near_nook = nook(their_strip, end)

    rest = []
    for p in range(slots):
        west, east, south, north = jump1[p * 4 : p * 4 + 4]
        mixed = (
            jnp.where(low, south, 0.0) + jnp.where(high, pltpu.roll(north, n - 1, 1), 0.0),
            jnp.where(low, pltpu.roll(south, 1, 1), 0.0) + jnp.where(high, north, 0.0),
            jnp.where(low, west, 0.0) + jnp.where(high, pltpu.roll(east, n - 1, 1), 0.0),
            jnp.where(low, pltpu.roll(west, 1, 1), 0.0) + jnp.where(high, east, 0.0),
        )
        for side in range(4):
            s = p * 4 + side
            rest.append(-mixed[side] - 2.0 * jump1[s] - lines2[s])

    settle(gather, recv_sem.at[1])

    def report(off):
        if simple:
            return gather[(me ^ away(off)) - 1, 1:]
        return gather[total - off - 1, 1:]

    reports = [whole(mine[1:])] + [whole(report(off)) for off in reach[1:]]
    value = look(reports, far_seat, far_nook)
    own = look(reports[:close], base, near_nook)
    bend = jnp.where((far_owner >= 0) & used, weight * (value - own), 0.0)
    best = [mine[:1]] + [gather[d, :1] for d in range(total - 1)]
    while len(best) > 1:
        best = [jnp.maximum(*best[k : k + 2]) if k + 1 < len(best) else best[k]
                for k in range(0, len(best), 2)]
    square = jnp.broadcast_to(jnp.max(best[0], axis=1, keepdims=True), (ROWS, n))
    step = (cfl_number / (n - 1)) * lax.rsqrt(square)
    half = 0.5 * step * step
    factors[0] = step
    factors[1] = half
    for p in range(slots):
        factors[2 + p] = jnp.where(count[0] > p, 1.0, 0.0) + jnp.zeros((ROWS, n), jnp.float32)
    early = [step * jump1[s] + half * along[s] for s in range(sides)]
    for s in range(sides):
        rest[s] = rest[s] + jnp.where(edge, pltpu.roll(bend, n - (2 * s + 1), 1), 0.0)

    settle(carried(inbox2, comps), recv_sem.at[2])
    other = partners(turned2, inbox2)
    jump2 = [
        early[s] + jnp.where(linked[s], (half * weight) * (other[s] + rest[s]), 0.0)
        for s in range(sides)
    ]
    spread(jump2)
    for s in range(sides):
        edges2[s] = jump2[s]

    settle(tally, send_sem.at[0])


def finish(fld, rate1, rate2, cols, edges2, factors, out_hbm, out_v, sem):
    comps, slots, n, _ = fld.shape
    chunks = n // ROWS
    lane = lax.broadcasted_iota(jnp.int32, (ROWS, n), 1)
    row = lax.broadcasted_iota(jnp.int32, (ROWS, n), 0)
    edge = (lane == 0) | (lane == n - 1)
    step, half = factors[0], factors[1]
    for p in range(slots):
        live = factors[2 + p] > 0.0
        for f in range(comps):
            for c in range(chunks):
                rows = pl.ds(c * ROWS, ROWS)
                side = pltpu.roll(cols[rows, :], n - (2 * (p * 8 + f) + 1), 1)
                value = fld[f, p, rows, :] + step * rate1[f, p, rows, :]
                value = value + half * rate2[f, p, rows, :] + jnp.where(edge, side, 0.0)
                for side, at in ((0, 0), (1, chunks - 1)):
                    if c == at:
                        line = jnp.broadcast_to(edges2[p * 4 + side, pl.ds(f, 1), :], (ROWS, n))
                        value = value + jnp.where(row == side * (ROWS - 1), line, 0.0)
                out_v[f, p, rows, :] = jnp.where(live, value, 0.0)
                if (c + 1) % 4 == 0:
                    part = (f, p, pl.ds((c - 3) * ROWS, 4 * ROWS))
                    pltpu.make_async_copy(out_v.at[part], out_hbm.at[part], sem.at[0]).start()
    pltpu.make_async_copy(out_v, out_hbm, sem.at[0]).wait()


def shards(
    total, subs, fields, density, moduli, metric_diag, metric_cross, extension, count, connectivity
):
    comps, slots, n, _ = fields.shape
    consts = circulant(n, extension.shape[0])
    far = total // 2 + 1
    offsets = (1, total - 1, far, total - far)
    reach = [0, *offsets]
    for a in offsets:
        for b in offsets:
            if (a + b) % total not in reach:
                reach.append((a + b) % total)
    f32, i32 = jnp.float32, jnp.int32
    hbm = pl.BlockSpec(memory_space=pltpu.HBM)
    state = pltpu.VMEM(fields.shape, f32)
    square = pltpu.VMEM((n, n), f32)
    dma = pltpu.SemaphoreType.DMA
    boxed = pltpu.VMEM((len(offsets) * slots, 8, n), f32)
    strips = pltpu.VMEM((slots * 4, 8, n), f32)
    factors = pltpu.VMEM((2 + slots, ROWS, n), f32)
    vmem = pl.BlockSpec(memory_space=pltpu.VMEM)
    parts = pl.pallas_call(
        functools.partial(kernel, total, subs, offsets, reach),
        out_shape=[state, state, state, square, strips, factors],
        in_specs=[hbm] * 9,
        out_specs=[vmem] * 6,
        scratch_shapes=[
            pltpu.SMEM(connectivity.shape[::-1], i32),
            pltpu.SMEM(count.shape, i32),
            pltpu.VMEM(extension.shape[::-1], f32),
            pltpu.VMEM(consts.shape, f32),
            pltpu.VMEM((7,) + density.shape, f32),
            state, state,
            pltpu.VMEM((2 * n, 2 * n), jnp.bfloat16),
            pltpu.VMEM((2 * n, 2 * n), jnp.bfloat16),
            pltpu.VMEM((-(-extension.shape[1] // ROWS) * ROWS, consts.shape[0] - n), f32),
            square,
            pltpu.VMEM((n, n), jnp.bfloat16),
            pltpu.VMEM((n, comps * slots * n), jnp.bfloat16),
            pltpu.VMEM((n, comps * slots * n), jnp.bfloat16),
            strips, strips,
            strips, strips, strips, strips,
            boxed, boxed, boxed, boxed,
            pltpu.VMEM((2, n), f32),
            pltpu.VMEM((total - 1, 2, n), f32),
            pltpu.VMEM((total - 1 + len(offsets) * slots * (2 * comps + 1) // 2, 2, n), f32),
            dma((6,)), dma((1,)), dma((3,)),
        ],
        compiler_params=pltpu.CompilerParams(collective_id=0, has_side_effects=True),
    )(connectivity.T, count, fields, density, moduli, metric_diag, metric_cross, extension.T,
      jnp.asarray(consts))
    return pl.pallas_call(
        finish,
        out_shape=jax.ShapeDtypeStruct(fields.shape, f32),
        in_specs=[vmem] * 6,
        out_specs=hbm,
        scratch_shapes=[state, dma((1,))],
        compiler_params=pltpu.CompilerParams(vmem_limit_bytes=8 * 2**20),
    )(*parts)


def solution(mesh):
    placed = (
        P(None, ("patch", "sub"), None, None),
        P(("patch", "sub"), None, None),
        P(None, ("patch", "sub"), None, None),
        P(None, ("patch", "sub"), None, None),
        P(None, ("patch", "sub"), None, None),
        P(),
        P(("patch", "sub")),
        P(("patch", "sub"), None),
    )
    total = mesh.shape["patch"] * mesh.shape["sub"]
    return jax.shard_map(
        functools.partial(shards, total, mesh.shape["sub"]),
        mesh=mesh,
        in_specs=placed,
        out_specs=P(None, ("patch", "sub"), None, None),
        check_vma=False,
    )
```
